512 devices in a mesh: dp: 16 (over z_lo, x), tensor: 32 (over z_hi, y, core).
Axes of the slice: x: 4, y: 8, z: 8 (z_hi: 2, z_lo: 4; z = z_hi * 4 + z_lo), core: 2. Of those that a mesh axis runs over, the one named last changes fastest.
Arguments:
- calibration: bfloat16 [4096, 6144], P('dp'), may hold values from -60 to 60
- expert_ids: int32 [4096, 2], P('dp'), may hold values from 0 to 7, all different within a row; in each aligned block of 256 rows (0 to 255, 256 to 511, ...) at most 80 rows name the same one
- chosen_expert: int32 [1], replicated, may hold values from 0 to 7
- ratio_ids: int32 [10], replicated, may hold values from 0 to 19
- gate_weight: bfloat16 [6144, 16384], P('dp', 'tensor'), may hold values from -0.078125 to 0.078125
Outputs:
- col_loss: float32 [10, 16384], P(None, 'tensor')
- losses: float32 [10], replicated
- best_loss: float32 [1], replicated
The draws below stay inside these ranges and needn't reach their ends.
Inputs may be any that keep to these rules, and one draw needn't show every extreme that they name: `expert_ids`: each row names two different experts; in the rows of one device no expert is named by more than 80 rows, a bound that some block reaches; every expert is named by some row.
All inputs are finite; a program needn't handle non-finite values.
Results may differ from the reference program's by a relative error of at most 0.0044.
Values may be sent and summed in bfloat16 or wider, within the bound.
A program may use at most 128 MiB of HBM per device.

```python
import math
import jax
import jax.numpy as jnp
import numpy as np
from jax import lax

D = 6144
FF = 16384
EXPERTS = 8
TOK_DEV = 256
RATIOS = 10
GRID = 20
GROUP = 128
CAP = 80
TOKENS = 4096
N_DP = 16


def draw_calibration(key, part):
    first, second = jax.random.split(key, 2)
    channel_scale = jnp.exp(jax.random.uniform(first, (D,), jnp.float32, -2.0, 2.0))
    values = jnp.clip(jax.random.normal(second, (TOKENS, D), jnp.float32), -6.0, 6.0)
    return (values * channel_scale[None, :]).astype(jnp.bfloat16)


def touch_ends(result, rng, low, largest):
    longest = result.shape.index(max(result.shape))
    spots = []
    for shift in (0, 1):
        where = [jax.random.randint(jax.random.fold_in(rng, axis), (), 0, length) for axis, length in enumerate(result.shape)]
        where[longest] = (where[longest] + shift) % result.shape[longest]
        spots.append(tuple(where))
    return result.at[spots[0]].set(low).at[spots[1]].set(largest)


def steps_of(rng, dims, cuts, low, high):
    loudness, own = 1.0, jax.random.fold_in(rng, 6)
    for dim, blocks in cuts:
        heights = jnp.exp(jax.random.uniform(jax.random.fold_in(own, dim), (blocks,), jnp.float32, low / len(cuts), high / len(cuts)))
        loudness = loudness * jnp.repeat(heights, dims[dim] // blocks).reshape([-1 if axis == dim else 1 for axis in range(len(dims))])
    return loudness


def assign_block(stream_key, own, number, rows, count, top, most, skew):
    ranking = jax.random.permutation(stream_key, count)
    crowded, ordinary = portions_of(count, rows * top, most, skew, True), portions_of(count, rows * top, most, skew, False)
    places = jnp.arange(count)

    def named(lengths, turn):
        used = int((lengths > 0).sum())
        fixed = max(1, used // 4)
        passed = fixed + (places - fixed + turn * (used - fixed)) % max(1, count - fixed)
        return jnp.zeros((count,), jnp.int32).at[ranking[jnp.where(places < fixed, places, passed)]].set(jnp.asarray(lengths, jnp.int32))

    lengths = jnp.where(number % 4 == 0, named(crowded, number // 4), named(ordinary, number - number // 4 - 1))
    mixed = jax.random.permutation(jax.random.fold_in(own, 3), count)
    source_of, receiver = mixed[0:count // 2 * 2:2], mixed[1:count // 2 * 2:2]
    room = jnp.minimum(lengths[source_of] - 1, most - lengths[receiver]) // 2
    room = jnp.where((source_of == ranking[0]) | (receiver == ranking[0]) | (lengths[receiver] == 0), 0, jnp.maximum(room, 0))
    passed = jax.random.randint(jax.random.fold_in(own, 4), (count // 2,), 0, 1 << 20) % (room + 1)
    lengths = lengths.at[source_of].add(-passed).at[receiver].add(passed)
    items = jnp.searchsorted(jnp.cumsum(lengths), jnp.arange(rows * top), side="right").astype(jnp.int32)
    grid = items.reshape(top, rows).T
    grid = grid[jax.random.permutation(jax.random.fold_in(own, 1), rows)]
    turn = jax.random.randint(jax.random.fold_in(own, 2), (rows, 1), 0, top)
    return jnp.take_along_axis(grid, (jnp.arange(top)[None, :] + turn) % top, axis=1)


def portions_of(number_of, total, most, lean, full):
    portions = [(1 << 20) // math.isqrt(standing ** lean) + 1 for standing in range(1, number_of + 1)]
    largest = most if full else min(most, max(-(-total // number_of), total * portions[0] // sum(portions)))
    least = 1 if total - largest >= number_of - 1 else 0
    counts, spare = [largest] + [least] * (number_of - 1), total - largest - least * (number_of - 1)
    while spare > 0:
        movable = [i for i in range(1, number_of) if counts[i] < largest] or [i for i in range(1, number_of) if counts[i] < most]
        mass, remaining = sum([portions[i] for i in movable]), spare
        for i in movable:
            extra = min(most - counts[i], max(1, remaining * portions[i] // mass), spare)
            counts[i] = counts[i] + extra
            spare = spare - extra
    return np.array(counts)


def noise(own_key, extent, width, most, shards=(), held_as=jnp.bfloat16):
    factor_of = steps_of(own_key, extent, shards, -0.22, 0.18) if shards else 1.0
    drawn = jax.random.normal(own_key, extent, jnp.float32) * width * factor_of
    return jnp.minimum(jnp.maximum(drawn, -most), most).astype(held_as)


def setup_inputs(seed: int = 0) -> dict:
    arg_keys = jax.random.split(jax.random.key(seed), 6)
    calibration = draw_calibration(jax.random.fold_in(arg_keys[5], 71), 0)
    expert_ids_keys = jax.random.split(jax.random.fold_in(arg_keys[1], 1), TOKENS // TOK_DEV)
    expert_ids_turns = jax.random.permutation(jax.random.fold_in(arg_keys[1], 3), TOKENS // TOK_DEV)
    expert_ids = jax.vmap(lambda own, number: assign_block(jax.random.fold_in(arg_keys[1], 2), own, number, TOK_DEV, EXPERTS, 2, CAP, 1))(expert_ids_keys, expert_ids_turns).reshape((TOKENS, 2))
    chosen_expert = jax.random.randint(arg_keys[2], (1,), 0, EXPERTS).astype(jnp.int32)
    ratio_ids = touch_ends(jax.random.randint(arg_keys[3], (RATIOS,), 0, GRID), jax.random.fold_in(arg_keys[3], 1), 0, GRID - 1).astype(jnp.int32)
    gate_weight = noise(arg_keys[4], (D, FF), D ** -0.5, 0.078125, ((0, 16), (1, 32)))
    return dict(calibration=calibration, expert_ids=expert_ids, chosen_expert=chosen_expert, ratio_ids=ratio_ids, gate_weight=gate_weight)


LEVELS = 7.0
LOSS_SCALE = 100.0


def pick_rows(expert_rows, block, expert, capacity):
    hit = jnp.any(expert_rows == expert, axis=1)
    position = jnp.cumsum(hit.astype(jnp.int32)) - 1
    slots = jnp.arange(capacity, dtype=jnp.int32)
    selected = hit[None, :] & (position[None, :] == slots[:, None])
    order = jnp.arange(block.shape[0], dtype=jnp.int32)
    row_index = jnp.sum(jnp.where(selected, order[None, :], 0), axis=1).astype(jnp.int32)
    occupied = jnp.any(selected, axis=1)
    routed = jnp.where(occupied[:, None], jnp.take(block, row_index, axis=0), jnp.zeros((), block.dtype))
    return routed, occupied


def error_matrix(weight, channel_sum, ratio):
    exponent = ratio.astype(jnp.float32) / GRID
    scales = jnp.exp(exponent * jnp.log(channel_sum))
    scaled = weight.astype(jnp.float32) * scales[:, None]
    grouped = scaled.reshape(weight.shape[0] // GROUP, GROUP, weight.shape[1])
    step_size = (jnp.max(jnp.abs(grouped), axis=1) + 1e-6) / LEVELS
    phase = grouped / step_size[:, None, :]
    error = (-step_size[:, None, :] / (2.0 * math.pi)) * jnp.sin(2.0 * math.pi * phase)
    return (error.reshape(weight.shape) / scales[:, None]).astype(jnp.bfloat16)


def reference(calibration, expert_ids, chosen_expert, ratio_ids, gate_weight):
    blocks = calibration.reshape(N_DP, TOK_DEV, D)
    id_blocks = expert_ids.reshape(N_DP, TOK_DEV, 2)
    routed, occupied = jax.vmap(lambda ids, block: pick_rows(ids, block, chosen_expert[0], CAP))(id_blocks, blocks)
    routed = routed.reshape(N_DP * CAP, D)
    token_count = jnp.sum(occupied.astype(jnp.float32))
    channel_sum = 0.001 + jnp.sum(jnp.abs(routed.astype(jnp.float32)), axis=0)
    routed_wide = routed.astype(jnp.float32)

    def per_ratio(ratio):
        error = error_matrix(gate_weight, channel_sum, ratio)
        product = jnp.dot(routed_wide, error.astype(jnp.float32))
        return LOSS_SCALE * jnp.sum(product * product, axis=0) / token_count

    col_loss = lax.map(per_ratio, ratio_ids)
    losses = jnp.sum(col_loss, axis=1) / FF
    best_loss = jnp.min(losses)[None]
    return col_loss, losses, best_loss
```

```python
import functools
import math

import jax
import jax.numpy as jnp
from jax import lax
from jax.experimental import pallas as pl
from jax.experimental.pallas import tpu as pltpu
from jax.sharding import PartitionSpec as P

FF = 16384
GRID = 20
GROUP = 128
CAP = 80
RATIOS = 10
LOSS_SCALE = 100.0
MESH = pl.DeviceIdType.MESH
VMEM = pl.BlockSpec(memory_space=pltpu.VMEM)
SMEM = pl.BlockSpec(memory_space=pltpu.SMEM)
DMA = pltpu.SemaphoreType.DMA

SINE = (
    6.283182818554192,
    -41.34142139892848,
    81.59618387812884,
    -76.58010057012196,
    41.20539503311958,
    -12.271262584796501,
)
SCALED = tuple(-c / (14.0 * math.pi) for c in SINE)


def params(**more):
    return pltpu.CompilerParams(vmem_limit_bytes=62 * 1024 * 1024, **more)


def place():
    dp, tensor = lax.axis_index("dp"), lax.axis_index("tensor")
    zl, x = dp // 4, dp % 4
    zh, y, c = tensor // 16, (tensor // 2) % 8, tensor % 2
    return dp, tensor, zl, x, zh, y, c


def beside(dz):
    dp, tensor, zl, x, zh, y, c = place()
    z = (zh * 4 + zl + dz) % 8
    return {"dp": (z % 4) * 4 + x, "tensor": ((z // 4) * 8 + y) * 2 + c}


def dp_peers():
    return [(dz, dx) for dz in range(4) for dx in range(4) if (dz, dx) != (0, 0)]


def tensor_peers():
    return [(a, b, c) for a in range(2) for b in range(8) for c in range(2) if (a, b, c) != (0, 0, 0)]


def dp_peer(dz, dx):
    dp, tensor, zl, x, zh, y, c = place()
    return {"dp": ((zl + dz) % 4) * 4 + (x + dx) % 4, "tensor": tensor}


def tensor_peer(dh, dy, dc):
    dp, tensor, zl, x, zh, y, c = place()
    return {"dp": dp, "tensor": (((zh + dh) % 2) * 8 + (y + dy) % 8) * 2 + (c + dc) % 2}


def meet(peers):
    barrier = pltpu.get_barrier_semaphore()
    for peer in peers:
        pl.semaphore_signal(barrier, inc=1, device_id=peer, device_id_type=MESH)
    pl.semaphore_wait(barrier, len(peers))


def remote(src, dst, send, recv, peer):
    return pltpu.make_async_remote_copy(
        src_ref=src, dst_ref=dst, send_sem=send, recv_sem=recv, device_id=peer, device_id_type=MESH
    )


def pick_kernel(expert_ref, ids_ref, block_ref, routed_ref, sums_ref):
    tokens, width = block_ref.shape
    hit = jnp.any(ids_ref[...] == expert_ref[0], axis=0, keepdims=True)
    hit = jnp.broadcast_to(jnp.where(hit, 1.0, 0.0), (8, tokens)).astype(jnp.bfloat16)
    up_to = lax.broadcasted_iota(jnp.int32, (tokens, tokens), 0) <= lax.broadcasted_iota(
        jnp.int32, (tokens, tokens), 1
    )
    place_of = jnp.dot(hit, jnp.where(up_to, 1.0, 0.0).astype(jnp.bfloat16), preferred_element_type=jnp.float32)
    slots = lax.broadcasted_iota(jnp.int32, (CAP, tokens), 0).astype(jnp.float32) + 1.0
    wanted = jnp.where(place_of[:1] == slots, hit[:1].astype(jnp.float32), 0.0)
    one_hot = wanted.astype(jnp.bfloat16)
    part = 512

    def pick(k, _):
        at = pl.ds(pl.multiple_of(k * part, part), part)
        rows = jnp.dot(one_hot, block_ref[:, at], preferred_element_type=jnp.float32)
        routed_ref[:, at] = rows.astype(jnp.bfloat16)
        sums_ref[:, at] = jnp.sum(jnp.abs(rows), axis=0, keepdims=True)
        return 0

    lax.fori_loop(0, width // part, pick, 0)
    sums_ref[:, width:] = jnp.broadcast_to(jnp.sum(wanted), (1, 128))


def exchange_kernel(
    routed_ref, sums_ref, w_ref, gath_ref, total_ref, wg_ref, zsum, xsum,
    zs_send, zs_recv, xs_send, xs_recv, w_send, w_recv, g_send, g_recv, d_send, d_recv,
):
    dp, tensor, zl, x, zh, y, c = place()
    width = routed_ref.shape[1]
    half = width // 2
    sibling = tensor_peer(0, 0, 1)
    meet([dp_peer(*o) for o in dp_peers()] + [beside(dz) for dz in (1, 7, 2, 6)] + [sibling])

    sums = [
        remote(sums_ref, zsum.at[zl], zs_send.at[k], zs_recv.at[k], beside(dz))
        for k, dz in enumerate((1, 7, 2))
    ]
    for copy in sums:
        copy.start()
    weights = []
    for k, (dz, dx) in enumerate(dp_peers()):
        columns = pl.ds(pl.multiple_of(((zl + dz) % 4) * GROUP, GROUP), GROUP)
        weights.append(remote(w_ref.at[:, columns], wg_ref.at[dp], w_send.at[k], w_recv.at[k], dp_peer(dz, dx)))
        weights[-1].start()
    rows = []
    low = c * half
    for k, (dz, start, size) in enumerate(((1, 0, half), (7, 0, half), (2, 0, half // 2), (6, half // 2, half // 2))):
        at = pl.ds(pl.multiple_of(low + start, GROUP), size)
        rows.append(remote(routed_ref.at[:, at], gath_ref.at[zl, :, at], g_send.at[k], g_recv.at[k], beside(dz)))
        rows[-1].start()

    zsum[zl] = sums_ref[...]
    for copy in sums:
        copy.wait_recv()
    xsum[x] = ((zsum[0] + zsum[1]) + zsum[2]) + zsum[3]
    across = [
        remote(xsum.at[x], xsum.at[x], xs_send.at[k], xs_recv.at[k], dp_peer(0, dx))
        for k, dx in enumerate((1, 3, 2))
    ]
    for copy in across:
        copy.start()
    gath_ref[zl] = routed_ref[...]
    wg_ref[dp] = w_ref[:, pl.ds(pl.multiple_of(zl * GROUP, GROUP), GROUP)]
    for copy in across:
        copy.wait_recv()
    total_ref[...] = ((xsum[0] + xsum[1]) + xsum[2]) + xsum[3]

    mine = pl.ds(pl.multiple_of(low, GROUP), half)
    passed = []
    for k, (arrived, back) in enumerate((((0,), 3), ((1,), 1), ((2, 3), 2))):
        for one in arrived:
            rows[one].wait_recv()
        held = gath_ref.at[(zl + back) % 4, :, mine]
        passed.append(remote(held, held, d_send.at[k], d_recv.at[k], sibling))
        passed[-1].start()
    for copy in weights:
        copy.wait_recv()
    for copy in passed:
        copy.wait_recv()
    for copy in sums + weights + rows + across + passed:
        copy.wait_send()


def errors_of(w7, aw, s, rs):
    t = jnp.max(aw * s, axis=1, keepdims=True) + 1e-6
    u = (w7 * s) * (1.0 / t)
    x = u - jnp.round(u)
    z = x * x
    p = z * SCALED[5] + SCALED[4]
    for c in SCALED[3::-1]:
        p = p * z + c
    return ((x * t) * rs * p).astype(jnp.bfloat16)


def search_kernel(ratio_ref, g_ref, total_ref, w_ref, out_ref, aw, w7, s_ref, rs_ref, err, acc):
    depth, cols = w_ref.shape
    rows = g_ref.shape[0]
    groups, width = 8, 512

    def turn(k, _):
        at = pl.ds(pl.multiple_of(k * GROUP, GROUP), GROUP)
        tile = w_ref[at, :].astype(jnp.float32).T
        aw[:, at] = jnp.abs(tile)
        w7[:, at] = 7.0 * tile
        return 0

    lax.fori_loop(0, depth // GROUP, turn, 0)
    logs = jnp.log(0.001 + total_ref[:, :depth])
    for r in range(RATIOS):
        s = jnp.exp((ratio_ref[r].astype(jnp.float32) / GRID) * logs)
        s_ref[r] = s
        rs_ref[r] = 1.0 / s

    def fill(i, _):
        r, k = i // (depth // GROUP // groups), i % (depth // GROUP // groups)
        for h in range(groups):
            at = pl.ds(pl.multiple_of((k * groups + h) * GROUP, GROUP), GROUP)
            err[pl.ds(pl.multiple_of(r * cols, cols), cols), at] = errors_of(
                w7[:, at], aw[:, at], s_ref[r, :, at], rs_ref[r, :, at]
            )
        return 0

    lax.fori_loop(0, RATIOS * (depth // GROUP // groups), fill, 0)
    acc[...] = jnp.zeros_like(acc)

    def multiply(k, _):
        at = pl.ds(pl.multiple_of(k * width, GROUP), width)
        acc[...] += lax.dot_general(
            err[:, at], g_ref[:, at], (((1,), (1,)), ((), ())), preferred_element_type=jnp.float32
        )
        return 0

    lax.fori_loop(0, depth // width, multiply, 0)
    factor = LOSS_SCALE / total_ref[:, depth:]
    for r in range(RATIOS):
        a = acc[r * cols : (r + 1) * cols, :]
        a = a * a
        folded = a[:, :128] + a[:, 128:256]
        folded = folded.T
        rest = a[:, 256:rows].T
        out_ref[r : r + 1, :] = factor * (
            jnp.sum(folded, axis=0, keepdims=True) + jnp.sum(rest, axis=0, keepdims=True)
        )
    out_ref[RATIOS:, :] = jnp.zeros((16 - RATIOS, cols), jnp.float32)


def close_kernel(part_ref, col_ref, losses_ref, best_ref, parts, sums, p_send, p_recv, l_send, l_recv):
    dp, tensor, zl, x, zh, y, c = place()
    meet([dp_peer(*o) for o in dp_peers()] + [tensor_peer(*o) for o in tensor_peers()])
    pieces = [
        remote(part_ref, parts.at[dp], p_send.at[k], p_recv.at[k], dp_peer(*o)) for k, o in enumerate(dp_peers())
    ]
    for copy in pieces:
        copy.start()
    parts[dp] = part_ref[...]
    for copy in pieces:
        copy.wait_recv()
    held = jnp.zeros((16, 1), jnp.float32)
    for q in range(4):
        piece = ((parts[4 * q] + parts[4 * q + 1]) + parts[4 * q + 2]) + parts[4 * q + 3]
        col_ref[:, q * 128 : (q + 1) * 128] = piece[:RATIOS]
        held = held + jnp.sum(piece, axis=1, keepdims=True)
    diagonal = lax.broadcasted_iota(jnp.int32, (16, 128), 0) == lax.broadcasted_iota(jnp.int32, (16, 128), 1)
    sums[tensor] = jnp.sum(jnp.where(diagonal, held, 0.0), axis=0, keepdims=True)
    rows = [
        remote(sums.at[tensor], sums.at[tensor], l_send.at[k], l_recv.at[k], tensor_peer(*o))
        for k, o in enumerate(tensor_peers())
    ]
    for copy in rows:
        copy.start()
    for copy in rows:
        copy.wait_recv()
    losses = jnp.sum(sums[...], axis=0) / FF
    losses_ref[...] = losses
    lane = lax.broadcasted_iota(jnp.int32, (1, 128), 1)
    best = jnp.min(jnp.where(lane < RATIOS, losses, jnp.inf), axis=1, keepdims=True)
    best_ref[...] = jnp.broadcast_to(best, (1, 128))
    for copy in pieces + rows:
        copy.wait_send()


def body(calibration, expert_ids, chosen_expert, ratio_ids, gate_weight):
    f32, bf16 = jnp.float32, jnp.bfloat16
    width = calibration.shape[1]
    slab, cols = gate_weight.shape
    long = width + 128
    routed, sums = pl.pallas_call(
        pick_kernel,
        out_shape=[jax.ShapeDtypeStruct((CAP, width), bf16), jax.ShapeDtypeStruct((1, long), f32)],
        in_specs=[SMEM, VMEM, VMEM],
        out_specs=[VMEM, VMEM],
        compiler_params=params(),
        name="pick",
    )(chosen_expert, expert_ids.T, calibration)
    gathered, total, columns = pl.pallas_call(
        exchange_kernel,
        out_shape=[
            jax.ShapeDtypeStruct((4, CAP, width), bf16),
            jax.ShapeDtypeStruct((1, long), f32),
            jax.ShapeDtypeStruct((16, slab, cols // 4), bf16),
        ],
        in_specs=[VMEM] * 3,
        out_specs=[VMEM] * 3,
        scratch_shapes=[
            pltpu.VMEM((4, 1, long), f32), pltpu.VMEM((4, 1, long), f32),
            DMA((3,)), DMA((3,)), DMA((3,)), DMA((3,)), DMA((15,)), DMA((15,)), DMA((4,)), DMA((4,)), DMA((3,)), DMA((3,)),
        ],
        compiler_params=params(collective_id=0, has_side_effects=True),
        name="exchange",
    )(routed, sums, gate_weight)
    part = pl.pallas_call(
        search_kernel,
        out_shape=jax.ShapeDtypeStruct((16, cols // 4), f32),
        in_specs=[SMEM, VMEM, VMEM, VMEM],
        out_specs=VMEM,
        scratch_shapes=[
            pltpu.VMEM((cols // 4, width), f32), pltpu.VMEM((cols // 4, width), f32),
            pltpu.VMEM((RATIOS, 1, width), f32), pltpu.VMEM((RATIOS, 1, width), f32),
            pltpu.VMEM((RATIOS * cols // 4, width), bf16), pltpu.VMEM((RATIOS * cols // 4, 4 * CAP), f32),
        ],
        compiler_params=params(),
        name="search",
    )(ratio_ids, gathered.reshape(4 * CAP, width), total, columns.reshape(16 * slab, cols // 4))
    col_loss, losses, best = pl.pallas_call(
        close_kernel,
        out_shape=[
            jax.ShapeDtypeStruct((RATIOS, cols), f32),
            jax.ShapeDtypeStruct((1, 128), f32),
            jax.ShapeDtypeStruct((1, 128), f32),
        ],
        in_specs=[VMEM],
        out_specs=[VMEM] * 3,
        scratch_shapes=[
            pltpu.VMEM((16, 16, 128), f32), pltpu.VMEM((32, 1, 128), f32),
            DMA((15,)), DMA((15,)), DMA((31,)), DMA((31,)),
        ],
        compiler_params=params(collective_id=1, has_side_effects=True),
        name="close",
    )(part)
    return col_loss, losses[0, :RATIOS], best[0, :1]


def solution(mesh):
    placed = (P("dp", None), P("dp", None), P(), P(), P("dp", "tensor"))
    return jax.shard_map(
        body, mesh=mesh, in_specs=placed, out_specs=(P(None, "tensor"), P(), P()), check_vma=False
    )
```

```python
import functools
import math

import jax
import jax.numpy as jnp
from jax import lax
from jax.experimental import pallas as pl
from jax.experimental.pallas import tpu as pltpu
from jax.sharding import PartitionSpec as P

FF = 16384
GRID = 20
GROUP = 128
CAP = 80
RATIOS = 10
LOSS_SCALE = 100.0
MESH = pl.DeviceIdType.MESH
VMEM = pl.BlockSpec(memory_space=pltpu.VMEM)
SMEM = pl.BlockSpec(memory_space=pltpu.SMEM)
DMA = pltpu.SemaphoreType.DMA

SINE = (
    6.283182818554192,
    -41.34142139892848,
    81.59618387812884,
    -76.58010057012196,
    41.20539503311958,
    -12.271262584796501,
)
SCALED = tuple(-c / (14.0 * math.pi) for c in SINE)


def params(**more):
    return pltpu.CompilerParams(vmem_limit_bytes=62 * 1024 * 1024, **more)


def place():
    dp, tensor = lax.axis_index("dp"), lax.axis_index("tensor")
    zl, x = dp // 4, dp % 4
    zh, y, c = tensor // 16, (tensor // 2) % 8, tensor % 2
    return dp, tensor, zl, x, zh, y, c


def beside(dz):
    dp, tensor, zl, x, zh, y, c = place()
    z = (zh * 4 + zl + dz) % 8
    return {"dp": (z % 4) * 4 + x, "tensor": ((z // 4) * 8 + y) * 2 + c}


def dp_peers():
    return [(dz, dx) for dz in range(4) for dx in range(4) if (dz, dx) != (0, 0)]


def tensor_peers():
    return [(a, b, c) for a in range(2) for b in range(8) for c in range(2) if (a, b, c) != (0, 0, 0)]


def dp_peer(dz, dx):
    dp, tensor, zl, x, zh, y, c = place()
    return {"dp": ((zl + dz) % 4) * 4 + (x + dx) % 4, "tensor": tensor}


def tensor_peer(dh, dy, dc):
    dp, tensor, zl, x, zh, y, c = place()
    return {"dp": dp, "tensor": (((zh + dh) % 2) * 8 + (y + dy) % 8) * 2 + (c + dc) % 2}


def remote(src, dst, send, recv, peer):
    return pltpu.make_async_remote_copy(
        src_ref=src, dst_ref=dst, send_sem=send, recv_sem=recv, device_id=peer, device_id_type=MESH
    )


def pick(expert_ref, ids_ref, block_ref, routed_ref, sums_ref):
    tokens, width = block_ref.shape
    hit = jnp.any(ids_ref[...] == expert_ref[0], axis=0, keepdims=True)
    hit = jnp.broadcast_to(jnp.where(hit, 1.0, 0.0), (8, tokens)).astype(jnp.bfloat16)
    up_to = lax.broadcasted_iota(jnp.int32, (tokens, tokens), 0) <= lax.broadcasted_iota(
        jnp.int32, (tokens, tokens), 1
    )
    place_of = jnp.dot(hit, jnp.where(up_to, 1.0, 0.0).astype(jnp.bfloat16), preferred_element_type=jnp.float32)
    slots = lax.broadcasted_iota(jnp.int32, (CAP, tokens), 0).astype(jnp.float32) + 1.0
    wanted = jnp.where(place_of[:1] == slots, hit[:1].astype(jnp.float32), 0.0)
    one_hot = wanted.astype(jnp.bfloat16)
    part = 1536

    def step(k, _):
        at = pl.ds(pl.multiple_of(k * part, part), part)
        rows = jnp.dot(one_hot, block_ref[:, at], preferred_element_type=jnp.float32)
        routed_ref[:, at] = rows.astype(jnp.bfloat16)
        sums_ref[:, at] = jnp.sum(jnp.abs(rows), axis=0, keepdims=True)
        return 0

    lax.fori_loop(0, width // part, step, 0)
    sums_ref[:, width:] = jnp.broadcast_to(jnp.sum(wanted), (1, 128))


def errors_of(w7, aw, s, rs):
    t = jnp.max(aw * s, axis=1, keepdims=True) + 1e-6
    u = (w7 * s) * (1.0 / t)
    x = u - jnp.round(u)
    z = x * x
    p = z * SCALED[5] + SCALED[4]
    for c in SCALED[3::-1]:
        p = p * z + c
    return ((x * t) * rs * p).astype(jnp.bfloat16)


def kernel(
    expert_ref, ratio_ref, ids_ref, block_ref, w_ref, col_ref, losses_ref, best_ref,
    gath, wg, zsum, xsum, aw, w7, s_ref, rs_ref, err, acc, parts, lsum,
    zs_send, zs_recv, xs_send, xs_recv, a_send, a_recv, b_send, b_recv, f_send, f_recv,
    g_send, g_recv, d_send, d_recv, p_send, p_recv, l_send, l_recv,
):
    dp, tensor, zl, x, zh, y, c = place()
    depth = block_ref.shape[1]
    slab, cols = w_ref.shape[0], w_ref.shape[1] // 4
    half = depth // 2
    sibling = tensor_peer(0, 0, 1)
    peers = [dp_peer(*o) for o in dp_peers()] + [beside(dz) for dz in (1, 7, 2, 6)]
    peers += [tensor_peer(*o) for o in tensor_peers()]
    barrier = pltpu.get_barrier_semaphore()
    for peer in peers:
        pl.semaphore_signal(barrier, inc=1, device_id=peer, device_id_type=MESH)

    def rows_of(block):
        return pl.ds(pl.multiple_of(block * CAP, 16), CAP)

    pick(expert_ref, ids_ref, block_ref, gath.at[rows_of(zl)], zsum.at[zl])
    wg[x, zl] = w_ref[:, pl.ds(pl.multiple_of(zl * cols, cols), cols)]
    pl.semaphore_wait(barrier, len(peers))

    sums = [remote(zsum.at[zl], zsum.at[zl], zs_send.at[k], zs_recv.at[k], beside(dz)) for k, dz in enumerate((1, 7, 2))]
    for copy in sums:
        copy.start()
    along = []
    for k, dz in enumerate((1, 3, 2)):
        columns = pl.ds(pl.multiple_of(((zl + dz) % 4) * cols, cols), cols)
        along.append(remote(w_ref.at[:, columns], wg.at[x, zl], a_send.at[k], a_recv.at[k], dp_peer(dz, 0)))
        along[-1].start()
    beyond = {}

    def across(j):
        held = wg.at[x, (zl + j) % 4]
        for k, dx in enumerate((1, 3)):
            beyond[j, dx] = remote(held, held, b_send.at[2 * j + k], b_recv.at[2 * j + k], dp_peer(0, dx))
            beyond[j, dx].start()

    across(0)
    rows = []
    low = c * half
    for k, (dz, start, size) in enumerate(((1, 0, half), (7, 0, half), (2, 0, half // 2), (6, half // 2, half // 2))):
        at = pl.ds(pl.multiple_of(low + start, GROUP), size)
        held = gath.at[rows_of(zl), at]
        rows.append(remote(held, held, g_send.at[k], g_recv.at[k], beside(dz)))
        rows[-1].start()

    for copy in sums:
        copy.wait_recv()
    xsum[x] = ((zsum[0] + zsum[1]) + zsum[2]) + zsum[3]
    over = [remote(xsum.at[x], xsum.at[x], xs_send.at[k], xs_recv.at[k], dp_peer(0, dx)) for k, dx in enumerate((1, 3, 2))]
    for copy in over:
        copy.start()
    for k, dz in ((0, 1), (1, 3), (2, 2)):
        along[k].wait_recv()
        across((4 - dz) % 4)

    def turn(column):
        def step(i, _):
            for h in range(slab // GROUP):
                tile = wg[column, i, h * GROUP : (h + 1) * GROUP, :].astype(jnp.float32).T
                at = pl.ds(pl.multiple_of((i * 4 + column) * slab + h * GROUP, GROUP), GROUP)
                aw[:, at] = jnp.abs(tile)
                w7[:, at] = 7.0 * tile
            return 0

        lax.fori_loop(0, 4, step, 0)

    def fill(column, first, last):
        def step(r, _):
            for i in range(4):
                for h in range(slab // GROUP):
                    at = pl.ds(pl.multiple_of((i * 4 + column) * slab + h * GROUP, GROUP), GROUP)
                    err[pl.ds(pl.multiple_of(r * cols, cols), cols), at] = errors_of(
                        w7[:, at], aw[:, at], s_ref[r, :, at], rs_ref[r, :, at]
                    )
            return 0

        lax.fori_loop(first, last, step, 0)

    turn(x)
    for copy in over:
        copy.wait_recv()
    total = ((xsum[0] + xsum[1]) + xsum[2]) + xsum[3]
    logs = jnp.log(0.001 + total[:, :depth])
    count = total[:, depth:]
    for r in range(RATIOS):
        s = jnp.exp((ratio_ref[r].astype(jnp.float32) / GRID) * logs)
        s_ref[r] = s
        rs_ref[r] = 1.0 / s

    fill(x, 0, 7)
    onward = []
    behind, ahead = (x + 3) % 4, (x + 1) % 4
    for k, (j, dx, column) in enumerate(((0, 1, behind), (1, 1, behind), (2, 3, ahead), (3, 3, ahead))):
        beyond[j, dx].wait_recv()
        held = wg.at[column, (zl + j) % 4]
        onward.append(remote(held, held, f_send.at[k], f_recv.at[k], dp_peer(0, dx)))
        onward[-1].start()
    fill(x, 7, RATIOS)
    for j in (2, 3):
        beyond[j, 1].wait_recv()
    turn(behind)
    fill(behind, 0, RATIOS)
    for j in (0, 1):
        beyond[j, 3].wait_recv()
    turn(ahead)
    fill(ahead, 0, RATIOS)
    mine = pl.ds(pl.multiple_of(low, GROUP), half)
    passed = []

    def pass_on(k, arrived, back):
        for one in arrived:
            rows[one].wait_recv()
        held = gath.at[rows_of((zl + back) % 4), mine]
        passed.append(remote(held, held, d_send.at[k], d_recv.at[k], sibling))
        passed[-1].start()

    pass_on(0, (0,), 3)
    pass_on(1, (1,), 1)
    for copy in onward:
        copy.wait_recv()
    far = (x + 2) % 4
    turn(far)
    fill(far, 0, 7)
    pass_on(2, (2, 3), 2)
    fill(far, 7, RATIOS)
    for copy in passed:
        copy.wait_recv()

    acc[...] = jnp.zeros_like(acc)
    part = depth // 4

    def multiply(k, _):
        at = pl.ds(pl.multiple_of(k * part, part), part)
        acc[...] += lax.dot_general(
            gath[:, at], err[:, at], (((1,), (1,)), ((), ())), preferred_element_type=jnp.float32
        )
        return 0

    lax.fori_loop(0, 4, multiply, 0)
    factor = LOSS_SCALE / count
    own = parts.at[dp]
    for r in range(RATIOS):
        a = acc[:, r * cols : (r + 1) * cols]
        own[r : r + 1, :] = factor * jnp.sum(a * a, axis=0, keepdims=True)
    own[RATIOS:, :] = jnp.zeros((16 - RATIOS, cols), jnp.float32)

    pieces = [remote(own, own, p_send.at[k], p_recv.at[k], dp_peer(*o)) for k, o in enumerate(dp_peers())]
    for copy in pieces:
        copy.start()
    for copy in pieces:
        copy.wait_recv()
    held = jnp.zeros((16, 1), jnp.float32)
    for q in range(4):
        piece = ((parts[4 * q] + parts[4 * q + 1]) + parts[4 * q + 2]) + parts[4 * q + 3]
        col_ref[:, q * cols : (q + 1) * cols] = piece[:RATIOS]
        held = held + jnp.sum(piece, axis=1, keepdims=True)
    diagonal = lax.broadcasted_iota(jnp.int32, (16, 128), 0) == lax.broadcasted_iota(jnp.int32, (16, 128), 1)
    lsum[tensor] = jnp.sum(jnp.where(diagonal, held, 0.0), axis=0, keepdims=True)
    shares = [
        remote(lsum.at[tensor], lsum.at[tensor], l_send.at[k], l_recv.at[k], tensor_peer(*o))
        for k, o in enumerate(tensor_peers())
    ]
    for copy in shares:
        copy.start()
    for copy in shares:
        copy.wait_recv()
    losses = jnp.sum(lsum[...], axis=0) / FF
    losses_ref[...] = losses
    lane = lax.broadcasted_iota(jnp.int32, (1, 128), 1)
    best = jnp.min(jnp.where(lane < RATIOS, losses, jnp.inf), axis=1, keepdims=True)
    best_ref[...] = jnp.broadcast_to(best, (1, 128))
    for copy in sums + along + list(beyond.values()) + rows + over + onward + passed + pieces + shares:
        copy.wait_send()


def body(calibration, expert_ids, chosen_expert, ratio_ids, gate_weight):
    f32, bf16 = jnp.float32, jnp.bfloat16
    width = calibration.shape[1]
    slab, cols = gate_weight.shape
    long, cols = width + 128, cols // 4
    col_loss, losses, best = pl.pallas_call(
        kernel,
        out_shape=[
            jax.ShapeDtypeStruct((RATIOS, 4 * cols), f32),
            jax.ShapeDtypeStruct((1, 128), f32),
            jax.ShapeDtypeStruct((1, 128), f32),
        ],
        in_specs=[SMEM, SMEM, VMEM, VMEM, VMEM],
        out_specs=[VMEM] * 3,
        scratch_shapes=[
            pltpu.VMEM((4 * CAP, width), bf16),
            pltpu.VMEM((4, 4, slab, cols), bf16),
            pltpu.VMEM((4, 1, long), f32),
            pltpu.VMEM((4, 1, long), f32),
            pltpu.VMEM((cols, width), f32),
            pltpu.VMEM((cols, width), f32),
            pltpu.VMEM((RATIOS, 1, width), f32),
            pltpu.VMEM((RATIOS, 1, width), f32),
            pltpu.VMEM((RATIOS * cols, width), bf16),
            pltpu.VMEM((4 * CAP, RATIOS * cols), f32),
            pltpu.VMEM((16, 16, cols), f32),
            pltpu.VMEM((32, 1, 128), f32),
        ]
        + [DMA((n,)) for n in (3, 3, 3, 3, 3, 3, 8, 8, 4, 4, 4, 4, 3, 3, 15, 15, 31, 31)],
        compiler_params=params(collective_id=0, has_side_effects=True),
        name="search",
    )(chosen_expert, ratio_ids, expert_ids.T, calibration, gate_weight)
    return col_loss, losses[0, :RATIOS], best[0, :1]


def solution(mesh):
    placed = (P("dp", None), P("dp", None), P(), P(), P("dp", "tensor"))
    return jax.shard_map(
        body, mesh=mesh, in_specs=placed, out_specs=(P(None, "tensor"), P(), P()), check_vma=False
    )
```

```python
import itertools
import math

import jax
import jax.numpy as jnp
from jax import lax
from jax.experimental import pallas as pl
from jax.experimental.pallas import tpu as pltpu
from jax.sharding import PartitionSpec as P

FF = 16384
GRID = 20
GROUP = 128
CAP = 80
RATIOS = 10
LOSS_SCALE = 100.0
MESH = pl.DeviceIdType.MESH
VMEM = pl.BlockSpec(memory_space=pltpu.VMEM)
SMEM = pl.BlockSpec(memory_space=pltpu.SMEM)
ANY = pl.BlockSpec(memory_space=pl.ANY)
DMA = pltpu.SemaphoreType.DMA

SINE = (
    6.283182818554192,
    -41.34142139892848,
    81.59618387812884,
    -76.58010057012196,
    41.20539503311958,
    -12.271262584796501,
)
SCALED = tuple(-c / (14.0 * math.pi) for c in SINE)


def params(**more):
    return pltpu.CompilerParams(vmem_limit_bytes=62 * 1024 * 1024, **more)


def place():
    dp, tensor = lax.axis_index("dp"), lax.axis_index("tensor")
    zl, x = dp // 4, dp % 4
    zh, y, c = tensor // 16, (tensor // 2) % 8, tensor % 2
    return dp, tensor, zl, x, zh, y, c


def others(*sizes):
    return [o for o in itertools.product(*(range(n) for n in sizes)) if any(o)]


def plane_peer(dz, dx):
    dp, tensor, zl, x, zh, y, c = place()
    z = (zh * 4 + zl + dz) % 8
    return {"dp": (z % 4) * 4 + (x + dx) % 4, "tensor": ((z // 4) * 8 + y) * 2 + c}


def dp_peer(dz, dx):
    dp, tensor, zl, x, zh, y, c = place()
    return {"dp": ((zl + dz) % 4) * 4 + (x + dx) % 4, "tensor": tensor}


def line_peer(dy, dc):
    dp, tensor, zl, x, zh, y, c = place()
    return {"dp": dp, "tensor": (zh * 8 + (y + dy) % 8) * 2 + (c + dc) % 2}


def remote(src, dst, send, recv, peer):
    return pltpu.make_async_remote_copy(
        src_ref=src, dst_ref=dst, send_sem=send, recv_sem=recv, device_id=peer, device_id_type=MESH
    )


def pick(expert_ref, ids_ref, block_ref, loads, routed_ref, sums_ref):
    tokens, width = block_ref.shape
    hit = jnp.any(ids_ref[...] == expert_ref[0], axis=0, keepdims=True)
    hit = jnp.broadcast_to(jnp.where(hit, 1.0, 0.0), (8, tokens)).astype(jnp.bfloat16)
    up_to = lax.broadcasted_iota(jnp.int32, (tokens, tokens), 0) <= lax.broadcasted_iota(
        jnp.int32, (tokens, tokens), 1
    )
    place_of = jnp.dot(hit, jnp.where(up_to, 1.0, 0.0).astype(jnp.bfloat16), preferred_element_type=jnp.float32)
    slots = lax.broadcasted_iota(jnp.int32, (CAP, tokens), 0).astype(jnp.float32) + 1.0
    wanted = jnp.where(place_of[:1] == slots, hit[:1].astype(jnp.float32), 0.0)
    one_hot = wanted.astype(jnp.bfloat16)
    part = width // len(loads)
    for k, load in enumerate(loads):
        load.wait()
        at = pl.ds(k * part, part)
        rows = jnp.dot(one_hot, block_ref[:, at], preferred_element_type=jnp.float32)
        routed_ref[:, at] = rows.astype(jnp.bfloat16)
        sums_ref[:, at] = jnp.sum(jnp.abs(rows), axis=0, keepdims=True)
    sums_ref[:, width:] = jnp.broadcast_to(jnp.sum(wanted), (1, 128))


def errors_of(w7, aw, s, rs):
    t = jnp.max(aw * s, axis=1, keepdims=True) + 1e-6
    u = (w7 * s) * (1.0 / t)
    x = u - jnp.round(u)
    z = x * x
    p = z * SCALED[5] + SCALED[4]
    for c in SCALED[3::-1]:
        p = p * z + c
    return ((x * t) * rs * p).astype(jnp.bfloat16)


def kernel(
    expert_ref, ratio_ref, ids_ref, block_hbm, w_hbm, col_ref, losses_ref, best_ref,
    block_ref, w_ref, gath, wg, zsum, xsum, aw, w7, s_ref, rs_ref, err, acc, parts, plane, line,
    load_sem,
    zs_send, zs_recv, xs_send, xs_recv, a_send, a_recv, b_send, b_recv, f_send, f_recv,
    g_send, g_recv, d_send, d_recv, p_send, p_recv, l_send, l_recv, m_send, m_recv,
):
    dp, tensor, zl, x, zh, y, c = place()
    depth = block_ref.shape[1]
    slab, cols = w_ref.shape[0], w_ref.shape[1] // 4
    half = depth // 2
    sibling = line_peer(0, 1)
    peers = [plane_peer(*o) for o in others(8, 4)] + [line_peer(*o) for o in others(8, 2)]
    barrier = pltpu.get_barrier_semaphore()
    for peer in peers:
        pl.semaphore_signal(barrier, inc=1, device_id=peer, device_id_type=MESH)
    part = depth // 4
    loads = [
        pltpu.make_async_copy(block_hbm.at[:, pl.ds(k * part, part)], block_ref.at[:, pl.ds(k * part, part)], load_sem.at[k])
        for k in range(4)
    ]
    weights = pltpu.make_async_copy(w_hbm, w_ref, load_sem.at[4])
    for load in loads + [weights]:
        load.start()

    def rows_of(block):
        return pl.ds(pl.multiple_of(block * CAP, 16), CAP)

    pick(expert_ref, ids_ref, block_ref, loads, gath.at[rows_of(zl)], zsum.at[zl])
    weights.wait()
    wg[x, zl] = w_ref[:, pl.ds(pl.multiple_of(zl * cols, cols), cols)]
    pl.semaphore_wait(barrier, len(peers))

    sums = [remote(zsum.at[zl], zsum.at[zl], zs_send.at[k], zs_recv.at[k], plane_peer(dz, 0)) for k, dz in enumerate((1, 7, 2))]
    for copy in sums:
        copy.start()
    along = []
    for k, dz in enumerate((1, 3, 2)):
        columns = pl.ds(pl.multiple_of(((zl + dz) % 4) * cols, cols), cols)
        along.append(remote(w_ref.at[:, columns], wg.at[x, zl], a_send.at[k], a_recv.at[k], dp_peer(dz, 0)))
        along[-1].start()
    beyond = {}

    def across(j):
        held = wg.at[x, (zl + j) % 4]
        for k, dx in enumerate((1, 3)):
            beyond[j, dx] = remote(held, held, b_send.at[2 * j + k], b_recv.at[2 * j + k], dp_peer(0, dx))
            beyond[j, dx].start()

    for copy in sums:
        copy.wait_recv()
    xsum[x] = ((zsum[0] + zsum[1]) + zsum[2]) + zsum[3]
    over = [remote(xsum.at[x], xsum.at[x], xs_send.at[k], xs_recv.at[k], dp_peer(0, dx)) for k, dx in enumerate((1, 3, 2))]
    for copy in over:
        copy.start()
    across(0)
    for k, dz in ((0, 1), (1, 3), (2, 2)):
        along[k].wait_recv()
        across((4 - dz) % 4)

    rows = []
    low = c * half
    for k, (dz, start, size) in enumerate(((1, 0, half), (7, 0, half), (2, 0, half // 2), (6, half // 2, half // 2))):
        at = pl.ds(pl.multiple_of(low + start, GROUP), size)
        held = gath.at[rows_of(zl), at]
        rows.append(remote(held, held, g_send.at[k], g_recv.at[k], plane_peer(dz, 0)))
        rows[-1].start()

    def turn(column):
        def step(i, _):
            for h in range(slab // GROUP):
                tile = wg[column, i, h * GROUP : (h + 1) * GROUP, :].astype(jnp.float32).T
                at = pl.ds(pl.multiple_of((i * 4 + column) * slab + h * GROUP, GROUP), GROUP)
                aw[:, at] = jnp.abs(tile)
                w7[:, at] = 7.0 * tile
            return 0

        lax.fori_loop(0, 4, step, 0)

    def fill(column, first, last):
        def step(r, _):
            for i in range(4):
                for h in range(slab // GROUP):
                    at = pl.ds(pl.multiple_of((i * 4 + column) * slab + h * GROUP, GROUP), GROUP)
                    err[pl.ds(pl.multiple_of(r * cols, cols), cols), at] = errors_of(
                        w7[:, at], aw[:, at], s_ref[r, :, at], rs_ref[r, :, at]
                    )
            return 0

        lax.fori_loop(first, last, step, 0)

    turn(x)
    for copy in over:
        copy.wait_recv()
    total = ((xsum[0] + xsum[1]) + xsum[2]) + xsum[3]
    logs = jnp.log(0.001 + total[:, :depth])
    count = total[:, depth:]
    for r in range(RATIOS):
        s = jnp.exp((ratio_ref[r].astype(jnp.float32) / GRID) * logs)
        s_ref[r] = s
        rs_ref[r] = 1.0 / s

    fill(x, 0, 7)
    onward = []
    behind, ahead = (x + 3) % 4, (x + 1) % 4
    for k, (j, dx, column) in enumerate(((0, 1, behind), (1, 1, behind), (2, 3, ahead), (3, 3, ahead))):
        beyond[j, dx].wait_recv()
        held = wg.at[column, (zl + j) % 4]
        onward.append(remote(held, held, f_send.at[k], f_recv.at[k], dp_peer(0, dx)))
        onward[-1].start()
    fill(x, 7, RATIOS)
    for j in (2, 3):
        beyond[j, 1].wait_recv()
    turn(behind)
    fill(behind, 0, RATIOS)
    for j in (0, 1):
        beyond[j, 3].wait_recv()
    turn(ahead)
    fill(ahead, 0, RATIOS)
    mine = pl.ds(pl.multiple_of(low, GROUP), half)
    passed = []

    def pass_on(k, arrived, back):
        for one in arrived:
            rows[one].wait_recv()
        held = gath.at[rows_of((zl + back) % 4), mine]
        passed.append(remote(held, held, d_send.at[k], d_recv.at[k], sibling))
        passed[-1].start()

    pass_on(0, (0,), 3)
    pass_on(1, (1,), 1)
    for copy in onward:
        copy.wait_recv()
    far = (x + 2) % 4
    turn(far)
    fill(far, 0, 7)
    pass_on(2, (2, 3), 2)
    fill(far, 7, RATIOS)
    for copy in passed:
        copy.wait_recv()

    acc[...] = jnp.zeros_like(acc)
    part = depth // 4

    def multiply(k, _):
        at = pl.ds(pl.multiple_of(k * part, part), part)
        acc[...] += lax.dot_general(
            gath[:, at], err[:, at], (((1,), (1,)), ((), ())), preferred_element_type=jnp.float32
        )
        return 0

    lax.fori_loop(0, 4, multiply, 0)
    factor = LOSS_SCALE / count
    own = parts.at[dp]
    for r in range(RATIOS):
        a = acc[:, r * cols : (r + 1) * cols]
        own[r : r + 1, :] = factor * jnp.sum(a * a, axis=0, keepdims=True)
    own[RATIOS:, :] = jnp.zeros((16 - RATIOS, cols), jnp.float32)

    pieces = [remote(own, own, p_send.at[k], p_recv.at[k], dp_peer(*o)) for k, o in enumerate(others(4, 4))]
    for copy in pieces:
        copy.start()
    diagonal = lax.broadcasted_iota(jnp.int32, (16, 128), 0) == lax.broadcasted_iota(jnp.int32, (16, 128), 1)
    row = plane.at[(zh * 4 + zl) * 4 + x]
    row[...] = jnp.sum(jnp.where(diagonal, jnp.sum(own[...], axis=1, keepdims=True), 0.0), axis=0, keepdims=True)
    shares = [remote(row, row, l_send.at[k], l_recv.at[k], plane_peer(*o)) for k, o in enumerate(others(8, 4))]
    for copy in shares:
        copy.start()
    for copy in shares:
        copy.wait_recv()
    row = line.at[y * 2 + c]
    row[...] = jnp.sum(plane[...], axis=0)
    ends = [remote(row, row, m_send.at[k], m_recv.at[k], line_peer(*o)) for k, o in enumerate(others(8, 2))]
    for copy in ends:
        copy.start()
    for copy in pieces:
        copy.wait_recv()
    for q in range(4):
        piece = ((parts[4 * q] + parts[4 * q + 1]) + parts[4 * q + 2]) + parts[4 * q + 3]
        col_ref[:, q * cols : (q + 1) * cols] = piece[:RATIOS]
    for copy in ends:
        copy.wait_recv()
    losses = jnp.sum(line[...], axis=0) / FF
    losses_ref[...] = losses
    lane = lax.broadcasted_iota(jnp.int32, (1, 128), 1)
    best = jnp.min(jnp.where(lane < RATIOS, losses, jnp.inf), axis=1, keepdims=True)
    best_ref[...] = jnp.broadcast_to(best, (1, 128))
    for copy in sums + along + list(beyond.values()) + rows + over + onward + passed + pieces + shares + ends:
        copy.wait_send()


def body(calibration, expert_ids, chosen_expert, ratio_ids, gate_weight):
    f32, bf16 = jnp.float32, jnp.bfloat16
    width = calibration.shape[1]
    slab, cols = gate_weight.shape
    long, cols = width + 128, cols // 4
    col_loss, losses, best = pl.pallas_call(
        kernel,
        out_shape=[
            jax.ShapeDtypeStruct((RATIOS, 4 * cols), f32),
            jax.ShapeDtypeStruct((1, 128), f32),
            jax.ShapeDtypeStruct((1, 128), f32),
        ],
        in_specs=[SMEM, SMEM, VMEM, ANY, ANY],
        out_specs=[VMEM] * 3,
        scratch_shapes=[
            pltpu.VMEM(calibration.shape, bf16),
            pltpu.VMEM((slab, 4 * cols), bf16),
            pltpu.VMEM((4 * CAP, width), bf16),
            pltpu.VMEM((4, 4, slab, cols), bf16),
            pltpu.VMEM((4, 1, long), f32),
            pltpu.VMEM((4, 1, long), f32),
            pltpu.VMEM((cols, width), f32),
            pltpu.VMEM((cols, width), f32),
            pltpu.VMEM((RATIOS, 1, width), f32),
            pltpu.VMEM((RATIOS, 1, width), f32),
            pltpu.VMEM((RATIOS * cols, width), bf16),
            pltpu.VMEM((4 * CAP, RATIOS * cols), f32),
            pltpu.VMEM((16, 16, cols), f32),
            pltpu.VMEM((32, 1, 128), f32),
            pltpu.VMEM((16, 1, 128), f32),
        ]
        + [DMA((n,)) for n in (5, 3, 3, 3, 3, 3, 3, 8, 8, 4, 4, 4, 4, 3, 3, 15, 15, 31, 31, 15, 15)],
        compiler_params=params(collective_id=0, has_side_effects=True),
        name="search",
    )(chosen_expert, ratio_ids, expert_ids.T, calibration, gate_weight)
    return col_loss, losses[0, :RATIOS], best[0, :1]


def solution(mesh):
    placed = (P("dp", None), P("dp", None), P(), P(), P("dp", "tensor"))
    return jax.shard_map(
        body, mesh=mesh, in_specs=placed, out_specs=(P(None, "tensor"), P(), P()), check_vma=False
    )
```

```python
import itertools
import math

import jax
import jax.numpy as jnp
from jax import lax
from jax.experimental import pallas as pl
from jax.experimental.pallas import tpu as pltpu
from jax.sharding import PartitionSpec as P

FF = 16384
GRID = 20
GROUP = 128
CAP = 80
RATIOS = 10
LOSS_SCALE = 100.0
MESH = pl.DeviceIdType.MESH
VMEM = pl.BlockSpec(memory_space=pltpu.VMEM)
SMEM = pl.BlockSpec(memory_space=pltpu.SMEM)
ANY = pl.BlockSpec(memory_space=pl.ANY)
DMA = pltpu.SemaphoreType.DMA

SINE = (
    6.283182818554192,
    -41.34142139892848,
    81.59618387812884,
    -76.58010057012196,
    41.20539503311958,
    -12.271262584796501,
)
MONIC = tuple(c / SINE[-1] for c in SINE[:-1])
LEADING = -SINE[-1] / (14.0 * math.pi)


def params(**more):
    return pltpu.CompilerParams(vmem_limit_bytes=62 * 1024 * 1024, **more)


def place():
    dp, tensor = lax.axis_index("dp"), lax.axis_index("tensor")
    zl, x = dp // 4, dp % 4
    zh, y, c = tensor // 16, (tensor // 2) % 8, tensor % 2
    return dp, tensor, zl, x, zh, y, c


def others(*sizes):
    return [o for o in itertools.product(*(range(n) for n in sizes)) if any(o)]


def plane_peer(dz, dx):
    dp, tensor, zl, x, zh, y, c = place()
    z = (zh * 4 + zl + dz) % 8
    return {"dp": (z % 4) * 4 + (x + dx) % 4, "tensor": ((z // 4) * 8 + y) * 2 + c}


def dp_peer(dz, dx):
    dp, tensor, zl, x, zh, y, c = place()
    return {"dp": ((zl + dz) % 4) * 4 + (x + dx) % 4, "tensor": tensor}


def line_peer(dy, dc):
    dp, tensor, zl, x, zh, y, c = place()
    return {"dp": dp, "tensor": (zh * 8 + (y + dy) % 8) * 2 + (c + dc) % 2}


def remote(src, dst, send, recv, peer):
    return pltpu.make_async_remote_copy(
        src_ref=src, dst_ref=dst, send_sem=send, recv_sem=recv, device_id=peer, device_id_type=MESH
    )


def pick(expert_ref, ids_ref, block_ref, loads, routed_ref, sums_ref):
    tokens, width = block_ref.shape
    hit = jnp.any(ids_ref[...] == expert_ref[0], axis=0, keepdims=True)
    hit = jnp.broadcast_to(jnp.where(hit, 1.0, 0.0), (8, tokens)).astype(jnp.bfloat16)
    up_to = lax.broadcasted_iota(jnp.int32, (tokens, tokens), 0) <= lax.broadcasted_iota(
        jnp.int32, (tokens, tokens), 1
    )
    place_of = jnp.dot(hit, jnp.where(up_to, 1.0, 0.0).astype(jnp.bfloat16), preferred_element_type=jnp.float32)
    slots = lax.broadcasted_iota(jnp.int32, (CAP, tokens), 0).astype(jnp.float32) + 1.0
    wanted = jnp.where(place_of[:1] == slots, hit[:1].astype(jnp.float32), 0.0)
    one_hot = wanted.astype(jnp.bfloat16)
    part = width // len(loads)
    for k, load in enumerate(loads):
        load.wait()
        at = pl.ds(k * part, part)
        rows = jnp.dot(one_hot, block_ref[:, at], preferred_element_type=jnp.float32)
        routed_ref[:, at] = rows.astype(jnp.bfloat16)
        sums_ref[:, at] = jnp.sum(jnp.abs(rows), axis=0, keepdims=True)
    sums_ref[:, width:] = jnp.broadcast_to(jnp.sum(wanted), (1, 128))


def errors_of(w7, aw, s, rs):
    t = jnp.max(aw * s, axis=1, keepdims=True) + 1e-6
    u = (w7 * s) * (1.0 / t)
    x = u - jnp.round(u)
    z = x * x
    p = z + MONIC[-1]
    for c in MONIC[-2::-1]:
        p = p * z + c
    return ((x * t) * rs * p).astype(jnp.bfloat16)


def kernel(
    expert_ref, ratio_ref, ids_ref, block_hbm, w_hbm, col_ref, losses_ref, best_ref,
    block_ref, w_ref, gath, wg, zsum, xsum, aw, w7, s_ref, rs_ref, err, acc, parts, plane, line,
    load_sem,
    zs_send, zs_recv, xs_send, xs_recv, a_send, a_recv, b_send, b_recv, f_send, f_recv,
    g_send, g_recv, d_send, d_recv, p_send, p_recv, l_send, l_recv, m_send, m_recv,
):
    dp, tensor, zl, x, zh, y, c = place()
    depth = block_ref.shape[1]
    slab, cols = w_ref.shape[0], w_ref.shape[1] // 4
    half = depth // 2
    sibling = line_peer(0, 1)
    peers = [plane_peer(*o) for o in others(8, 4)] + [line_peer(*o) for o in others(8, 2)]
    barrier = pltpu.get_barrier_semaphore()
    for peer in peers:
        pl.semaphore_signal(barrier, inc=1, device_id=peer, device_id_type=MESH)
    part = depth // 4
    loads = [
        pltpu.make_async_copy(block_hbm.at[:, pl.ds(k * part, part)], block_ref.at[:, pl.ds(k * part, part)], load_sem.at[k])
        for k in range(4)
    ]
    weights = pltpu.make_async_copy(w_hbm, w_ref, load_sem.at[4])
    for load in loads + [weights]:
        load.start()

    def rows_of(block):
        return pl.ds(pl.multiple_of(block * CAP, 16), CAP)

    pick(expert_ref, ids_ref, block_ref, loads, gath.at[rows_of(zl)], zsum.at[zl])
    weights.wait()
    wg[x, zl] = w_ref[:, pl.ds(pl.multiple_of(zl * cols, cols), cols)]
    pl.semaphore_wait(barrier, len(peers))

    sums = [remote(zsum.at[zl], zsum.at[zl], zs_send.at[k], zs_recv.at[k], plane_peer(dz, 0)) for k, dz in enumerate((1, 7, 2))]
    for copy in sums:
        copy.start()
    along = []
    for k, dz in enumerate((1, 3, 2)):
        columns = pl.ds(pl.multiple_of(((zl + dz) % 4) * cols, cols), cols)
        along.append(remote(w_ref.at[:, columns], wg.at[x, zl], a_send.at[k], a_recv.at[k], dp_peer(dz, 0)))
        along[-1].start()
    beyond = {}

    def across(j):
        held = wg.at[x, (zl + j) % 4]
        for k, dx in enumerate((1, 3)):
            beyond[j, dx] = remote(held, held, b_send.at[2 * j + k], b_recv.at[2 * j + k], dp_peer(0, dx))
            beyond[j, dx].start()

    for copy in sums:
        copy.wait_recv()
    xsum[x] = ((zsum[0] + zsum[1]) + zsum[2]) + zsum[3]
    over = [remote(xsum.at[x], xsum.at[x], xs_send.at[k], xs_recv.at[k], dp_peer(0, dx)) for k, dx in enumerate((1, 3, 2))]
    for copy in over:
        copy.start()
    across(0)
    for k, dz in ((0, 1), (1, 3), (2, 2)):
        along[k].wait_recv()
        across((4 - dz) % 4)

    rows = []
    low = c * half
    for k, (dz, start, size) in enumerate(((1, 0, half), (7, 0, half), (2, 0, half // 2), (6, half // 2, half // 2))):
        at = pl.ds(pl.multiple_of(low + start, GROUP), size)
        held = gath.at[rows_of(zl), at]
        rows.append(remote(held, held, g_send.at[k], g_recv.at[k], plane_peer(dz, 0)))
        rows[-1].start()

    def turn(column):
        def step(i, _):
            for h in range(slab // GROUP):
                tile = wg[column, i, h * GROUP : (h + 1) * GROUP, :].astype(jnp.float32).T
                at = pl.ds(pl.multiple_of((i * 4 + column) * slab + h * GROUP, GROUP), GROUP)
                aw[:, at] = jnp.abs(tile)
                w7[:, at] = 7.0 * tile
            return 0

        lax.fori_loop(0, 4, step, 0)

    def fill(column, first, last):
        def step(pair, _):
            for one in range(2):
                r = pair * 2 + one
                for i in range(4):
                    for h in range(slab // GROUP):
                        group = (i * 4 + column) * (slab // GROUP) + h
                        at = pl.ds(pl.multiple_of(group * GROUP, GROUP), GROUP)
                        err[group, pl.ds(pl.multiple_of(r * cols, cols), cols), :] = errors_of(
                            w7[:, at], aw[:, at], s_ref[r, :, at], rs_ref[r, :, at]
                        )
            return 0

        lax.fori_loop(first, last, step, 0)

    turn(x)
    for copy in over:
        copy.wait_recv()
    total = ((xsum[0] + xsum[1]) + xsum[2]) + xsum[3]
    logs = jnp.log(0.001 + total[:, :depth])
    count = total[:, depth:]
    for r in range(RATIOS):
        s = jnp.exp((ratio_ref[r].astype(jnp.float32) / GRID) * logs)
        s_ref[r] = s
        rs_ref[r] = LEADING / s

    fill(x, 0, 3)
    onward = []
    behind, ahead = (x + 3) % 4, (x + 1) % 4
    for k, (j, dx, column) in enumerate(((0, 1, behind), (1, 1, behind), (2, 3, ahead), (3, 3, ahead))):
        beyond[j, dx].wait_recv()
        held = wg.at[column, (zl + j) % 4]
        onward.append(remote(held, held, f_send.at[k], f_recv.at[k], dp_peer(0, dx)))
        onward[-1].start()
    fill(x, 3, RATIOS // 2)
    for j in (2, 3):
        beyond[j, 1].wait_recv()
    turn(behind)
    fill(behind, 0, RATIOS // 2)
    for j in (0, 1):
        beyond[j, 3].wait_recv()
    turn(ahead)
    fill(ahead, 0, RATIOS // 2)
    mine = pl.ds(pl.multiple_of(low, GROUP), half)
    passed = []

    def pass_on(k, arrived, back):
        for one in arrived:
            rows[one].wait_recv()
        held = gath.at[rows_of((zl + back) % 4), mine]
        passed.append(remote(held, held, d_send.at[k], d_recv.at[k], sibling))
        passed[-1].start()

    pass_on(0, (0,), 3)
    pass_on(1, (1,), 1)
    for copy in onward:
        copy.wait_recv()
    far = (x + 2) % 4
    turn(far)
    fill(far, 0, 3)
    pass_on(2, (2, 3), 2)
    fill(far, 3, RATIOS // 2)
    acc[...] = jnp.zeros_like(acc)

    def multiply(k, _):
        chunk = (k + 2 * c) % 4
        at = pl.ds(pl.multiple_of(chunk * part, part), part)
        groups = part // GROUP
        errors = jnp.concatenate([err[chunk * groups + j] for j in range(groups)], axis=1)
        acc[...] += lax.dot_general(
            gath[:, at], errors, (((1,), (1,)), ((), ())), preferred_element_type=jnp.float32
        )
        return 0

    lax.fori_loop(0, 2, multiply, 0)
    for copy in passed:
        copy.wait_recv()
    lax.fori_loop(2, 4, multiply, 0)
    factor = LOSS_SCALE / count
    own = parts.at[dp]
    for r in range(RATIOS):
        a = acc[:, r * cols : (r + 1) * cols]
        own[r : r + 1, :] = factor * jnp.sum(a * a, axis=0, keepdims=True)
    own[RATIOS:, :] = jnp.zeros((16 - RATIOS, cols), jnp.float32)

    pieces = [remote(own, own, p_send.at[k], p_recv.at[k], dp_peer(*o)) for k, o in enumerate(others(4, 4))]
    for copy in pieces:
        copy.start()
    diagonal = lax.broadcasted_iota(jnp.int32, (16, 128), 0) == lax.broadcasted_iota(jnp.int32, (16, 128), 1)
    row = plane.at[(zh * 4 + zl) * 4 + x]
    row[...] = jnp.sum(jnp.where(diagonal, jnp.sum(own[...], axis=1, keepdims=True), 0.0), axis=0, keepdims=True)
    shares = [remote(row, row, l_send.at[k], l_recv.at[k], plane_peer(*o)) for k, o in enumerate(others(8, 4))]
    for copy in shares:
        copy.start()
    for copy in shares:
        copy.wait_recv()
    row = line.at[y * 2 + c]
    row[...] = jnp.sum(plane[...], axis=0)
    ends = [remote(row, row, m_send.at[k], m_recv.at[k], line_peer(*o)) for k, o in enumerate(others(8, 2))]
    for copy in ends:
        copy.start()
    for copy in pieces:
        copy.wait_recv()
    for q in range(4):
        piece = ((parts[4 * q] + parts[4 * q + 1]) + parts[4 * q + 2]) + parts[4 * q + 3]
        col_ref[:, q * cols : (q + 1) * cols] = piece[:RATIOS]
    for copy in ends:
        copy.wait_recv()
    losses = jnp.sum(line[...], axis=0) / FF
    losses_ref[...] = losses
    lane = lax.broadcasted_iota(jnp.int32, (1, 128), 1)
    best = jnp.min(jnp.where(lane < RATIOS, losses, jnp.inf), axis=1, keepdims=True)
    best_ref[...] = jnp.broadcast_to(best, (1, 128))
    for copy in sums + along + list(beyond.values()) + rows + over + onward + passed + pieces + shares + ends:
        copy.wait_send()


def finish_kernel(col_ref, losses_ref, best_ref, col_out, losses_out, best_out):
    col_out[...] = col_ref[...]
    for r in range(RATIOS):
        losses_out[r] = losses_ref[0, r]
    best_out[0] = best_ref[0, 0]


def body(calibration, expert_ids, chosen_expert, ratio_ids, gate_weight):
    f32, bf16 = jnp.float32, jnp.bfloat16
    width = calibration.shape[1]
    slab, cols = gate_weight.shape
    long, cols = width + 128, cols // 4
    col_loss, losses, best = pl.pallas_call(
        kernel,
        out_shape=[
            jax.ShapeDtypeStruct((RATIOS, 4 * cols), f32),
            jax.ShapeDtypeStruct((1, 128), f32),
            jax.ShapeDtypeStruct((1, 128), f32),
        ],
        in_specs=[SMEM, SMEM, VMEM, ANY, ANY],
        out_specs=[VMEM] * 3,
        scratch_shapes=[
            pltpu.VMEM(calibration.shape, bf16),
            pltpu.VMEM((slab, 4 * cols), bf16),
            pltpu.VMEM((4 * CAP, width), bf16),
            pltpu.VMEM((4, 4, slab, cols), bf16),
            pltpu.VMEM((4, 1, long), f32),
            pltpu.VMEM((4, 1, long), f32),
            pltpu.VMEM((cols, width), f32),
            pltpu.VMEM((cols, width), f32),
            pltpu.VMEM((RATIOS, 1, width), f32),
            pltpu.VMEM((RATIOS, 1, width), f32),
            pltpu.VMEM((width // GROUP, RATIOS * cols, GROUP), bf16),
            pltpu.VMEM((4 * CAP, RATIOS * cols), f32),
            pltpu.VMEM((16, 16, cols), f32),
            pltpu.VMEM((32, 1, 128), f32),
            pltpu.VMEM((16, 1, 128), f32),
        ]
        + [DMA((n,)) for n in (5, 3, 3, 3, 3, 3, 3, 8, 8, 4, 4, 4, 4, 3, 3, 15, 15, 31, 31, 15, 15)],
        compiler_params=params(collective_id=0, has_side_effects=True),
        name="search",
    )(chosen_expert, ratio_ids, expert_ids.T, calibration, gate_weight)
    return pl.pallas_call(
        finish_kernel,
        out_shape=[
            jax.ShapeDtypeStruct((RATIOS, 4 * cols), f32),
            jax.ShapeDtypeStruct((RATIOS,), f32),
            jax.ShapeDtypeStruct((1,), f32),
        ],
        in_specs=[VMEM, SMEM, SMEM],
        out_specs=[VMEM, SMEM, SMEM],
        name="finish",
    )(col_loss, losses, best)


def solution(mesh):
    placed = (P("dp", None), P("dp", None), P(), P(), P("dp", "tensor"))
    return jax.shard_map(
        body, mesh=mesh, in_specs=placed, out_specs=(P(None, "tensor"), P(), P()), check_vma=False
    )
```

```python
import itertools
import math

import jax
import jax.numpy as jnp
from jax import lax
from jax.experimental import pallas as pl
from jax.experimental.pallas import tpu as pltpu
from jax.sharding import PartitionSpec as P

FF = 16384
GRID = 20
GROUP = 128
CAP = 80
RATIOS = 10
LOSS_SCALE = 100.0
MESH = pl.DeviceIdType.MESH
VMEM = pl.BlockSpec(memory_space=pltpu.VMEM)
SMEM = pl.BlockSpec(memory_space=pltpu.SMEM)
ANY = pl.BlockSpec(memory_space=pl.ANY)
DMA = pltpu.SemaphoreType.DMA

SINE = (
    6.283182818554192,
    -41.34142139892848,
    81.59618387812884,
    -76.58010057012196,
    41.20539503311958,
    -12.271262584796501,
)
MONIC = tuple(c / SINE[-1] for c in SINE[:-1])
LEADING = -SINE[-1] / (14.0 * math.pi)


def params(**more):
    return pltpu.CompilerParams(vmem_limit_bytes=62 * 1024 * 1024, **more)


def place():
    dp, tensor = lax.axis_index("dp"), lax.axis_index("tensor")
    zl, x = dp // 4, dp % 4
    zh, y, c = tensor // 16, (tensor // 2) % 8, tensor % 2
    return dp, tensor, zl, x, zh, y, c


def others(*sizes):
    return [o for o in itertools.product(*(range(n) for n in sizes)) if any(o)]


def plane_peer(dz, dx):
    dp, tensor, zl, x, zh, y, c = place()
    z = (zh * 4 + zl + dz) % 8
    return {"dp": (z % 4) * 4 + (x + dx) % 4, "tensor": ((z // 4) * 8 + y) * 2 + c}


def dp_peer(dz, dx):
    dp, tensor, zl, x, zh, y, c = place()
    return {"dp": ((zl + dz) % 4) * 4 + (x + dx) % 4, "tensor": tensor}


def line_peer(dy, dc):
    dp, tensor, zl, x, zh, y, c = place()
    return {"dp": dp, "tensor": (zh * 8 + (y + dy) % 8) * 2 + (c + dc) % 2}


def remote(src, dst, send, recv, peer):
    return pltpu.make_async_remote_copy(
        src_ref=src, dst_ref=dst, send_sem=send, recv_sem=recv, device_id=peer, device_id_type=MESH
    )


def pick(expert_ref, ids_ref, block_ref, loads, routed_ref, sums_ref):
    tokens, width = block_ref.shape
    hit = jnp.any(ids_ref[...] == expert_ref[0], axis=0, keepdims=True)
    hit = jnp.broadcast_to(jnp.where(hit, 1.0, 0.0), (8, tokens)).astype(jnp.bfloat16)
    up_to = lax.broadcasted_iota(jnp.int32, (tokens, tokens), 0) <= lax.broadcasted_iota(
        jnp.int32, (tokens, tokens), 1
    )
    place_of = jnp.dot(hit, jnp.where(up_to, 1.0, 0.0).astype(jnp.bfloat16), preferred_element_type=jnp.float32)
    slots = lax.broadcasted_iota(jnp.int32, (CAP, tokens), 0).astype(jnp.float32) + 1.0
    wanted = jnp.where(place_of[:1] == slots, hit[:1].astype(jnp.float32), 0.0)
    one_hot = wanted.astype(jnp.bfloat16)
    part = width // len(loads)
    for k, load in enumerate(loads):
        load.wait()
        at = pl.ds(k * part, part)
        rows = jnp.dot(one_hot, block_ref[:, at], preferred_element_type=jnp.float32)
        routed_ref[:, at] = rows.astype(jnp.bfloat16)
        sums_ref[:, at] = jnp.sum(jnp.abs(rows), axis=0, keepdims=True)
    sums_ref[:, width:] = jnp.broadcast_to(jnp.sum(wanted), (1, 128))


def errors_of(w7, aw, s, rs):
    t = jnp.max(aw * s, axis=1, keepdims=True) + 1e-6
    u = (w7 * s) * (1.0 / t)
    x = u - jnp.round(u)
    z = x * x
    p = z + MONIC[-1]
    for c in MONIC[-2::-1]:
        p = p * z + c
    return ((x * t) * rs * p).astype(jnp.bfloat16)


def kernel(
    expert_ref, ratio_ref, ids_ref, block_hbm, w_hbm, col_ref, losses_ref, best_ref,
    block_ref, w_ref, gath, wg, zsum, xsum, aw, w7, s_ref, rs_ref, err, acc, parts, plane, line,
    load_sem,
    zs_send, zs_recv, xs_send, xs_recv, a_send, a_recv, b_send, b_recv, f_send, f_recv,
    g_send, g_recv, d_send, d_recv, p_send, p_recv, l_send, l_recv, m_send, m_recv,
):
    dp, tensor, zl, x, zh, y, c = place()
    depth = block_ref.shape[1]
    slab, cols = w_ref.shape[0], w_ref.shape[1] // 4
    half = depth // 2
    sibling = line_peer(0, 1)
    peers = [plane_peer(*o) for o in others(8, 4)] + [line_peer(*o) for o in others(8, 2)]
    barrier = pltpu.get_barrier_semaphore()
    for peer in peers:
        pl.semaphore_signal(barrier, inc=1, device_id=peer, device_id_type=MESH)
    part = depth // 4
    loads = [
        pltpu.make_async_copy(block_hbm.at[:, pl.ds(k * part, part)], block_ref.at[:, pl.ds(k * part, part)], load_sem.at[k])
        for k in range(4)
    ]
    weights = pltpu.make_async_copy(w_hbm, w_ref, load_sem.at[4])
    for load in loads + [weights]:
        load.start()

    def rows_of(block):
        return pl.ds(pl.multiple_of(block * CAP, 16), CAP)

    pick(expert_ref, ids_ref, block_ref, loads, gath.at[rows_of(zl)], zsum.at[zl])
    weights.wait()
    wg[x, zl] = w_ref[:, pl.ds(pl.multiple_of(zl * cols, cols), cols)]
    pl.semaphore_wait(barrier, len(peers))

    sums = [remote(zsum.at[zl], zsum.at[zl], zs_send.at[k], zs_recv.at[k], plane_peer(dz, 0)) for k, dz in enumerate((1, 7, 2))]
    for copy in sums:
        copy.start()
    along = []
    for k, dz in enumerate((1, 3, 2)):
        columns = pl.ds(pl.multiple_of(((zl + dz) % 4) * cols, cols), cols)
        along.append(remote(w_ref.at[:, columns], wg.at[x, zl], a_send.at[k], a_recv.at[k], dp_peer(dz, 0)))
        along[-1].start()
    beyond = {}

    def across(j):
        held = wg.at[x, (zl + j) % 4]
        for k, dx in enumerate((1, 3)):
            beyond[j, dx] = remote(held, held, b_send.at[2 * j + k], b_recv.at[2 * j + k], dp_peer(0, dx))
            beyond[j, dx].start()

    for copy in sums:
        copy.wait_recv()
    xsum[x] = ((zsum[0] + zsum[1]) + zsum[2]) + zsum[3]
    over = [remote(xsum.at[x], xsum.at[x], xs_send.at[k], xs_recv.at[k], dp_peer(0, dx)) for k, dx in enumerate((1, 3, 2))]
    for copy in over:
        copy.start()
    across(0)
    acc[...] = jnp.zeros_like(acc)
    for k, dz in ((0, 1), (1, 3), (2, 2)):
        along[k].wait_recv()
        across((4 - dz) % 4)

    rows = []
    low = c * half
    for k, (dz, start, size) in enumerate(((1, 0, half), (7, 0, half), (2, 0, half // 2), (6, half // 2, half // 2))):
        at = pl.ds(pl.multiple_of(low + start, GROUP), size)
        held = gath.at[rows_of(zl), at]
        rows.append(remote(held, held, g_send.at[k], g_recv.at[k], plane_peer(dz, 0)))
        rows[-1].start()

    def turn(column):
        def step(i, _):
            for h in range(slab // GROUP):
                tile = wg[column, i, h * GROUP : (h + 1) * GROUP, :].astype(jnp.float32).T
                at = pl.ds(pl.multiple_of((i * 4 + column) * slab + h * GROUP, GROUP), GROUP)
                aw[:, at] = jnp.abs(tile)
                w7[:, at] = 7.0 * tile
            return 0

        lax.fori_loop(0, 4, step, 0)

    def fill(column, first, last):
        def step(pair, _):
            for one in range(2):
                r = pair * 2 + one
                for i in range(4):
                    for h in range(slab // GROUP):
                        group = (i * 4 + column) * (slab // GROUP) + h
                        at = pl.ds(pl.multiple_of(group * GROUP, GROUP), GROUP)
                        err[group, pl.ds(pl.multiple_of(r * cols, cols), cols), :] = errors_of(
                            w7[:, at], aw[:, at], s_ref[r, :, at], rs_ref[r, :, at]
                        )
            return 0

        lax.fori_loop(first, last, step, 0)

    turn(x)
    for copy in over:
        copy.wait_recv()
    total = ((xsum[0] + xsum[1]) + xsum[2]) + xsum[3]
    logs = jnp.log(0.001 + total[:, :depth])
    count = total[:, depth:]
    for r in range(RATIOS):
        s = jnp.exp((ratio_ref[r].astype(jnp.float32) / GRID) * logs)
        s_ref[r] = s
        rs_ref[r] = LEADING / s

    fill(x, 0, 3)
    onward = []
    behind, ahead = (x + 3) % 4, (x + 1) % 4
    for k, (j, dx, column) in enumerate(((0, 1, behind), (1, 1, behind), (2, 3, ahead), (3, 3, ahead))):
        beyond[j, dx].wait_recv()
        held = wg.at[column, (zl + j) % 4]
        onward.append(remote(held, held, f_send.at[k], f_recv.at[k], dp_peer(0, dx)))
        onward[-1].start()
    fill(x, 3, RATIOS // 2)
    for j in (2, 3):
        beyond[j, 1].wait_recv()
    turn(behind)
    fill(behind, 0, RATIOS // 2)
    for j in (0, 1):
        beyond[j, 3].wait_recv()
    turn(ahead)
    fill(ahead, 0, RATIOS // 2)
    mine = pl.ds(pl.multiple_of(low, GROUP), half)
    passed = []

    def pass_on(k, arrived, back):
        for one in arrived:
            rows[one].wait_recv()
        held = gath.at[rows_of((zl + back) % 4), mine]
        passed.append(remote(held, held, d_send.at[k], d_recv.at[k], sibling))
        passed[-1].start()

    pass_on(0, (0,), 3)
    pass_on(1, (1,), 1)
    for copy in onward:
        copy.wait_recv()
    far = (x + 2) % 4
    turn(far)
    fill(far, 0, 3)
    pass_on(2, (2, 3), 2)
    fill(far, 3, RATIOS // 2)
    def multiply(k, _):
        chunk = (k + 2 * c) % 4
        at = pl.ds(pl.multiple_of(chunk * part, part), part)
        groups = part // GROUP
        errors = jnp.concatenate([err[chunk * groups + j] for j in range(groups)], axis=1)
        acc[...] += lax.dot_general(
            gath[:, at], errors, (((1,), (1,)), ((), ())), preferred_element_type=jnp.float32
        )
        return 0

    lax.fori_loop(0, 2, multiply, 0)
    for copy in passed:
        copy.wait_recv()
    lax.fori_loop(2, 4, multiply, 0)
    factor = LOSS_SCALE / count
    own = parts.at[dp]
    for r in range(RATIOS):
        a = acc[:, r * cols : (r + 1) * cols]
        own[r : r + 1, :] = factor * jnp.sum(a * a, axis=0, keepdims=True)
    own[RATIOS:, :] = jnp.zeros((16 - RATIOS, cols), jnp.float32)

    pieces = [remote(own, own, p_send.at[k], p_recv.at[k], dp_peer(*o)) for k, o in enumerate(others(4, 4))]
    diagonal = lax.broadcasted_iota(jnp.int32, (16, 128), 0) == lax.broadcasted_iota(jnp.int32, (16, 128), 1)
    row = plane.at[(zh * 4 + zl) * 4 + x]
    row[...] = jnp.sum(jnp.where(diagonal, jnp.sum(own[...], axis=1, keepdims=True), 0.0), axis=0, keepdims=True)
    shares = [remote(row, row, l_send.at[k], l_recv.at[k], plane_peer(*o)) for k, o in enumerate(others(8, 4))]
    for copy in shares + pieces:
        copy.start()
    for copy in shares:
        copy.wait_recv()
    row = line.at[y * 2 + c]
    row[...] = jnp.sum(plane[...], axis=0)
    ends = [remote(row, row, m_send.at[k], m_recv.at[k], line_peer(*o)) for k, o in enumerate(others(8, 2))]
    for copy in ends:
        copy.start()
    for copy in pieces:
        copy.wait_recv()
    for q in range(4):
        piece = ((parts[4 * q] + parts[4 * q + 1]) + parts[4 * q + 2]) + parts[4 * q + 3]
        col_ref[:, q * cols : (q + 1) * cols] = piece[:RATIOS]
    for copy in ends:
        copy.wait_recv()
    losses = jnp.sum(line[...], axis=0) / FF
    losses_ref[...] = losses
    lane = lax.broadcasted_iota(jnp.int32, (1, 128), 1)
    best = jnp.min(jnp.where(lane < RATIOS, losses, jnp.inf), axis=1, keepdims=True)
    best_ref[...] = jnp.broadcast_to(best, (1, 128))
    for copy in sums + along + list(beyond.values()) + rows + over + onward + passed + pieces + shares + ends:
        copy.wait_send()


def finish_kernel(col_ref, losses_ref, best_ref, col_out, losses_out, best_out):
    col_out[...] = col_ref[...]
    for r in range(RATIOS):
        losses_out[r] = losses_ref[0, r]
    best_out[0] = best_ref[0, 0]


def body(calibration, expert_ids, chosen_expert, ratio_ids, gate_weight):
    f32, bf16 = jnp.float32, jnp.bfloat16
    width = calibration.shape[1]
    slab, cols = gate_weight.shape
    long, cols = width + 128, cols // 4
    col_loss, losses, best = pl.pallas_call(
        kernel,
        out_shape=[
            jax.ShapeDtypeStruct((RATIOS, 4 * cols), f32),
            jax.ShapeDtypeStruct((1, 128), f32),
            jax.ShapeDtypeStruct((1, 128), f32),
        ],
        in_specs=[SMEM, SMEM, VMEM, ANY, ANY],
        out_specs=[VMEM] * 3,
        scratch_shapes=[
            pltpu.VMEM(calibration.shape, bf16),
            pltpu.VMEM((slab, 4 * cols), bf16),
            pltpu.VMEM((4 * CAP, width), bf16),
            pltpu.VMEM((4, 4, slab, cols), bf16),
            pltpu.VMEM((4, 1, long), f32),
            pltpu.VMEM((4, 1, long), f32),
            pltpu.VMEM((cols, width), f32),
            pltpu.VMEM((cols, width), f32),
            pltpu.VMEM((RATIOS, 1, width), f32),
            pltpu.VMEM((RATIOS, 1, width), f32),
            pltpu.VMEM((width // GROUP, RATIOS * cols, GROUP), bf16),
            pltpu.VMEM((4 * CAP, RATIOS * cols), f32),
            pltpu.VMEM((16, 16, cols), f32),
            pltpu.VMEM((32, 1, 128), f32),
            pltpu.VMEM((16, 1, 128), f32),
        ]
        + [DMA((n,)) for n in (5, 3, 3, 3, 3, 3, 3, 8, 8, 4, 4, 4, 4, 3, 3, 15, 15, 31, 31, 15, 15)],
        compiler_params=params(collective_id=0, has_side_effects=True),
        name="search",
    )(chosen_expert, ratio_ids, expert_ids.T, calibration, gate_weight)
    return pl.pallas_call(
        finish_kernel,
        out_shape=[
            jax.ShapeDtypeStruct((RATIOS, 4 * cols), f32),
            jax.ShapeDtypeStruct((RATIOS,), f32),
            jax.ShapeDtypeStruct((1,), f32),
        ],
        in_specs=[VMEM, SMEM, SMEM],
        out_specs=[VMEM, SMEM, SMEM],
        name="finish",
    )(col_loss, losses, best)


def solution(mesh):
    placed = (P("dp", None), P("dp", None), P(), P(), P("dp", "tensor"))
    return jax.shard_map(
        body, mesh=mesh, in_specs=placed, out_specs=(P(None, "tensor"), P(), P()), check_vma=False
    )
```

```python
import itertools
import math

import jax
import jax.numpy as jnp
from jax import lax
from jax.experimental import pallas as pl
from jax.experimental.pallas import tpu as pltpu
from jax.sharding import PartitionSpec as P

FF = 16384
GRID = 20
GROUP = 128
CAP = 80
RATIOS = 10
LOSS_SCALE = 100.0
MESH = pl.DeviceIdType.MESH
VMEM = pl.BlockSpec(memory_space=pltpu.VMEM)
SMEM = pl.BlockSpec(memory_space=pltpu.SMEM)
ANY = pl.BlockSpec(memory_space=pl.ANY)
DMA = pltpu.SemaphoreType.DMA

SINE = (
    6.283182818554192,
    -41.34142139892848,
    81.59618387812884,
    -76.58010057012196,
    41.20539503311958,
    -12.271262584796501,
)
MONIC = tuple(c / SINE[-1] for c in SINE[:-1])
LEADING = -SINE[-1] / (14.0 * math.pi)


def params(**more):
    return pltpu.CompilerParams(vmem_limit_bytes=62 * 1024 * 1024, **more)


def place():
    dp, tensor = lax.axis_index("dp"), lax.axis_index("tensor")
    zl, x = dp // 4, dp % 4
    zh, y, c = tensor // 16, (tensor // 2) % 8, tensor % 2
    return dp, tensor, zl, x, zh, y, c


def others(*sizes):
    offsets = [o for o in itertools.product(*(range(n) for n in sizes)) if any(o)]
    return sorted(offsets, key=lambda o: -sum(min(i, n - i) for i, n in zip(o, sizes)))


def plane_peer(dz, dx):
    dp, tensor, zl, x, zh, y, c = place()
    z = (zh * 4 + zl + dz) % 8
    return {"dp": (z % 4) * 4 + (x + dx) % 4, "tensor": ((z // 4) * 8 + y) * 2 + c}


def dp_peer(dz, dx):
    dp, tensor, zl, x, zh, y, c = place()
    return {"dp": ((zl + dz) % 4) * 4 + (x + dx) % 4, "tensor": tensor}


def line_peer(dy, dc):
    dp, tensor, zl, x, zh, y, c = place()
    return {"dp": dp, "tensor": (zh * 8 + (y + dy) % 8) * 2 + (c + dc) % 2}


def remote(src, dst, send, recv, peer):
    return pltpu.make_async_remote_copy(
        src_ref=src, dst_ref=dst, send_sem=send, recv_sem=recv, device_id=peer, device_id_type=MESH
    )


def pick(expert_ref, ids_ref, block_ref, loads, routed_ref, sums_ref):
    tokens, width = block_ref.shape
    hit = jnp.any(ids_ref[...] == expert_ref[0], axis=0, keepdims=True)
    hit = jnp.broadcast_to(jnp.where(hit, 1.0, 0.0), (8, tokens)).astype(jnp.bfloat16)
    up_to = lax.broadcasted_iota(jnp.int32, (tokens, tokens), 0) <= lax.broadcasted_iota(
        jnp.int32, (tokens, tokens), 1
    )
    place_of = jnp.dot(hit, jnp.where(up_to, 1.0, 0.0).astype(jnp.bfloat16), preferred_element_type=jnp.float32)
    slots = lax.broadcasted_iota(jnp.int32, (CAP, tokens), 0).astype(jnp.float32) + 1.0
    wanted = jnp.where(place_of[:1] == slots, hit[:1].astype(jnp.float32), 0.0)
    one_hot = wanted.astype(jnp.bfloat16)
    part = width // len(loads)
    for k, load in enumerate(loads):
        load.wait()
        at = pl.ds(k * part, part)
        rows = jnp.dot(one_hot, block_ref[:, at], preferred_element_type=jnp.float32)
        routed_ref[:, at] = rows.astype(jnp.bfloat16)
        sums_ref[:, at] = jnp.sum(jnp.abs(rows), axis=0, keepdims=True)
    sums_ref[:, width:] = jnp.broadcast_to(jnp.sum(wanted), (1, 128))


def errors_of(w7, aw, s, rs):
    t = jnp.max(aw * s, axis=1, keepdims=True) + 1e-6
    u = (w7 * s) * (1.0 / t)
    x = u - jnp.round(u)
    z = x * x
    p = z + MONIC[-1]
    for c in MONIC[-2::-1]:
        p = p * z + c
    return ((x * t) * rs * p).astype(jnp.bfloat16)


def kernel(
    expert_ref, ratio_ref, ids_ref, block_hbm, w_hbm, col_ref, losses_ref, best_ref,
    block_ref, w_ref, gath, wg, zsum, xsum, aw, w7, s_ref, rs_ref, err, acc, parts, plane, line,
    load_sem,
    zs_send, zs_recv, xs_send, xs_recv, a_send, a_recv, b_send, b_recv, f_send, f_recv,
    g_send, g_recv, d_send, d_recv, p_send, p_recv, l_send, l_recv, m_send, m_recv,
):
    dp, tensor, zl, x, zh, y, c = place()
    depth = block_ref.shape[1]
    slab, cols = w_ref.shape[0], w_ref.shape[1] // 4
    half = depth // 2
    sibling = line_peer(0, 1)
    part = depth // 4
    loads = [
        pltpu.make_async_copy(block_hbm.at[:, pl.ds(k * part, part)], block_ref.at[:, pl.ds(k * part, part)], load_sem.at[k])
        for k in range(4)
    ]
    weights = pltpu.make_async_copy(w_hbm, w_ref, load_sem.at[4])
    for load in loads + [weights]:
        load.start()
    peers = [plane_peer(*o) for o in others(8, 4)] + [line_peer(*o) for o in others(8, 2)]
    barrier = pltpu.get_barrier_semaphore()
    for peer in peers:
        pl.semaphore_signal(barrier, inc=1, device_id=peer, device_id_type=MESH)

    def rows_of(block):
        return pl.ds(pl.multiple_of(block * CAP, 16), CAP)

    pick(expert_ref, ids_ref, block_ref, loads, gath.at[rows_of(zl)], zsum.at[zl])
    pl.semaphore_wait(barrier, len(peers))

    sums = [remote(zsum.at[zl], zsum.at[zl], zs_send.at[k], zs_recv.at[k], plane_peer(dz, 0)) for k, dz in enumerate((2, 1, 7))]
    for copy in sums:
        copy.start()
    weights.wait()
    along = []
    for k, dz in enumerate((1, 3, 2)):
        columns = pl.ds(pl.multiple_of(((zl + dz) % 4) * cols, cols), cols)
        along.append(remote(w_ref.at[:, columns], wg.at[x, zl], a_send.at[k], a_recv.at[k], dp_peer(dz, 0)))
        along[-1].start()
    wg[x, zl] = w_ref[:, pl.ds(pl.multiple_of(zl * cols, cols), cols)]
    beyond = {}

    def across(j):
        held = wg.at[x, (zl + j) % 4]
        for k, dx in enumerate((1, 3)):
            beyond[j, dx] = remote(held, held, b_send.at[2 * j + k], b_recv.at[2 * j + k], dp_peer(0, dx))
            beyond[j, dx].start()

    for copy in sums:
        copy.wait_recv()
    xsum[x] = ((zsum[0] + zsum[1]) + zsum[2]) + zsum[3]
    over = [remote(xsum.at[x], xsum.at[x], xs_send.at[k], xs_recv.at[k], dp_peer(0, dx)) for k, dx in enumerate((2, 1, 3))]
    for copy in over:
        copy.start()
    across(0)
    acc[...] = jnp.zeros_like(acc)
    for k, dz in ((0, 1), (1, 3), (2, 2)):
        along[k].wait_recv()
        across((4 - dz) % 4)

    rows = []
    low = c * half
    for k, (dz, start, size) in enumerate(((1, 0, half), (7, 0, half), (2, 0, half // 2), (6, half // 2, half // 2))):
        at = pl.ds(pl.multiple_of(low + start, GROUP), size)
        held = gath.at[rows_of(zl), at]
        rows.append(remote(held, held, g_send.at[k], g_recv.at[k], plane_peer(dz, 0)))
        rows[-1].start()

    def turn(column):
        def step(i, _):
            for h in range(slab // GROUP):
                tile = wg[column, i, h * GROUP : (h + 1) * GROUP, :].astype(jnp.float32).T
                at = pl.ds(pl.multiple_of((i * 4 + column) * slab + h * GROUP, GROUP), GROUP)
                aw[:, at] = jnp.abs(tile)
                w7[:, at] = 7.0 * tile
            return 0

        lax.fori_loop(0, 4, step, 0)

    def fill(column, first, last):
        def step(pair, _):
            for one in range(2):
                r = pair * 2 + one
                for i in range(4):
                    for h in range(slab // GROUP):
                        group = (i * 4 + column) * (slab // GROUP) + h
                        at = pl.ds(pl.multiple_of(group * GROUP, GROUP), GROUP)
                        err[group, pl.ds(pl.multiple_of(r * cols, cols), cols), :] = errors_of(
                            w7[:, at], aw[:, at], s_ref[r, :, at], rs_ref[r, :, at]
                        )
            return 0

        lax.fori_loop(first, last, step, 0)

    turn(x)
    for copy in over:
        copy.wait_recv()
    total = ((xsum[0] + xsum[1]) + xsum[2]) + xsum[3]
    logs = jnp.log(0.001 + total[:, :depth])
    count = total[:, depth:]
    for r in range(RATIOS):
        s = jnp.exp((ratio_ref[r].astype(jnp.float32) / GRID) * logs)
        s_ref[r] = s
        rs_ref[r] = LEADING / s

    fill(x, 0, 3)
    onward = []
    behind, ahead = (x + 3) % 4, (x + 1) % 4
    for k, (j, dx, column) in enumerate(((0, 1, behind), (1, 1, behind), (2, 3, ahead), (3, 3, ahead))):
        beyond[j, dx].wait_recv()
        held = wg.at[column, (zl + j) % 4]
        onward.append(remote(held, held, f_send.at[k], f_recv.at[k], dp_peer(0, dx)))
        onward[-1].start()
    fill(x, 3, RATIOS // 2)
    for j in (2, 3):
        beyond[j, 1].wait_recv()
    turn(behind)
    fill(behind, 0, RATIOS // 2)
    for j in (0, 1):
        beyond[j, 3].wait_recv()
    turn(ahead)
    fill(ahead, 0, RATIOS // 2)
    mine = pl.ds(pl.multiple_of(low, GROUP), half)
    passed = []

    def pass_on(k, arrived, back):
        for one in arrived:
            rows[one].wait_recv()
        held = gath.at[rows_of((zl + back) % 4), mine]
        passed.append(remote(held, held, d_send.at[k], d_recv.at[k], sibling))
        passed[-1].start()

    pass_on(0, (0,), 3)
    pass_on(1, (1,), 1)
    for copy in onward:
        copy.wait_recv()
    far = (x + 2) % 4
    turn(far)
    fill(far, 0, 3)
    pass_on(2, (2, 3), 2)
    fill(far, 3, RATIOS // 2)
    def multiply(k, _):
        chunk = (k + 2 * c) % 4
        at = pl.ds(pl.multiple_of(chunk * part, part), part)
        groups = part // GROUP
        errors = jnp.concatenate([err[chunk * groups + j] for j in range(groups)], axis=1)
        acc[...] += lax.dot_general(
            gath[:, at], errors, (((1,), (1,)), ((), ())), preferred_element_type=jnp.float32
        )
        return 0

    lax.fori_loop(0, 2, multiply, 0)
    for copy in passed:
        copy.wait_recv()
    lax.fori_loop(2, 4, multiply, 0)
    factor = LOSS_SCALE / count
    own = parts.at[dp]
    for r in range(RATIOS):
        a = acc[:, r * cols : (r + 1) * cols]
        own[r : r + 1, :] = factor * jnp.sum(a * a, axis=0, keepdims=True)
    own[RATIOS:, :] = jnp.zeros((16 - RATIOS, cols), jnp.float32)

    pieces = [remote(own, own, p_send.at[k], p_recv.at[k], dp_peer(*o)) for k, o in enumerate(others(4, 4))]
    diagonal = lax.broadcasted_iota(jnp.int32, (16, 128), 0) == lax.broadcasted_iota(jnp.int32, (16, 128), 1)
    row = plane.at[(zh * 4 + zl) * 4 + x]
    row[...] = jnp.sum(jnp.where(diagonal, jnp.sum(own[...], axis=1, keepdims=True), 0.0), axis=0, keepdims=True)
    shares = [remote(row, row, l_send.at[k], l_recv.at[k], plane_peer(*o)) for k, o in enumerate(others(8, 4))]
    for copy in shares + pieces:
        copy.start()
    for copy in shares:
        copy.wait_recv()
    row = line.at[y * 2 + c]
    row[...] = jnp.sum(plane[...], axis=0)
    ends = [remote(row, row, m_send.at[k], m_recv.at[k], line_peer(*o)) for k, o in enumerate(others(8, 2))]
    for copy in ends:
        copy.start()
    for copy in pieces:
        copy.wait_recv()
    for q in range(4):
        piece = ((parts[4 * q] + parts[4 * q + 1]) + parts[4 * q + 2]) + parts[4 * q + 3]
        col_ref[:, q * cols : (q + 1) * cols] = piece[:RATIOS]
    for copy in ends:
        copy.wait_recv()
    losses = jnp.sum(line[...], axis=0) / FF
    losses_ref[...] = losses
    lane = lax.broadcasted_iota(jnp.int32, (1, 128), 1)
    best = jnp.min(jnp.where(lane < RATIOS, losses, jnp.inf), axis=1, keepdims=True)
    best_ref[...] = jnp.broadcast_to(best, (1, 128))
    for copy in sums + along + list(beyond.values()) + rows + over + onward + passed + pieces + shares + ends:
        copy.wait_send()


def finish_kernel(col_ref, losses_ref, best_ref, col_out, losses_out, best_out):
    col_out[...] = col_ref[...]
    for r in range(RATIOS):
        losses_out[r] = losses_ref[0, r]
    best_out[0] = best_ref[0, 0]


def body(calibration, expert_ids, chosen_expert, ratio_ids, gate_weight):
    f32, bf16 = jnp.float32, jnp.bfloat16
    width = calibration.shape[1]
    slab, cols = gate_weight.shape
    long, cols = width + 128, cols // 4
    col_loss, losses, best = pl.pallas_call(
        kernel,
        out_shape=[
            jax.ShapeDtypeStruct((RATIOS, 4 * cols), f32),
            jax.ShapeDtypeStruct((1, 128), f32),
            jax.ShapeDtypeStruct((1, 128), f32),
        ],
        in_specs=[SMEM, SMEM, VMEM, ANY, ANY],
        out_specs=[VMEM] * 3,
        scratch_shapes=[
            pltpu.VMEM(calibration.shape, bf16),
            pltpu.VMEM((slab, 4 * cols), bf16),
            pltpu.VMEM((4 * CAP, width), bf16),
            pltpu.VMEM((4, 4, slab, cols), bf16),
            pltpu.VMEM((4, 1, long), f32),
            pltpu.VMEM((4, 1, long), f32),
            pltpu.VMEM((cols, width), f32),
            pltpu.VMEM((cols, width), f32),
            pltpu.VMEM((RATIOS, 1, width), f32),
            pltpu.VMEM((RATIOS, 1, width), f32),
            pltpu.VMEM((width // GROUP, RATIOS * cols, GROUP), bf16),
            pltpu.VMEM((4 * CAP, RATIOS * cols), f32),
            pltpu.VMEM((16, 16, cols), f32),
            pltpu.VMEM((32, 1, 128), f32),
            pltpu.VMEM((16, 1, 128), f32),
        ]
        + [DMA((n,)) for n in (5, 3, 3, 3, 3, 3, 3, 8, 8, 4, 4, 4, 4, 3, 3, 15, 15, 31, 31, 15, 15)],
        compiler_params=params(collective_id=0, has_side_effects=True),
        name="search",
    )(chosen_expert, ratio_ids, expert_ids.T, calibration, gate_weight)
    return pl.pallas_call(
        finish_kernel,
        out_shape=[
            jax.ShapeDtypeStruct((RATIOS, 4 * cols), f32),
            jax.ShapeDtypeStruct((RATIOS,), f32),
            jax.ShapeDtypeStruct((1,), f32),
        ],
        in_specs=[VMEM, SMEM, SMEM],
        out_specs=[VMEM, SMEM, SMEM],
        name="finish",
    )(col_loss, losses, best)


def solution(mesh):
    placed = (P("dp", None), P("dp", None), P(), P(), P("dp", "tensor"))
    return jax.shard_map(
        body, mesh=mesh, in_specs=placed, out_specs=(P(None, "tensor"), P(), P()), check_vma=False
    )
```

```python
import itertools
import math

import jax
import jax.numpy as jnp
from jax import lax
from jax.experimental import pallas as pl
from jax.experimental.pallas import tpu as pltpu
from jax.sharding import PartitionSpec as P

FF = 16384
GRID = 20
GROUP = 128
CAP = 80
RATIOS = 10
LOSS_SCALE = 100.0
MESH = pl.DeviceIdType.MESH
VMEM = pl.BlockSpec(memory_space=pltpu.VMEM)
SMEM = pl.BlockSpec(memory_space=pltpu.SMEM)
ANY = pl.BlockSpec(memory_space=pl.ANY)
DMA = pltpu.SemaphoreType.DMA

SINE = (
    6.283182818554192,
    -41.34142139892848,
    81.59618387812884,
    -76.58010057012196,
    41.20539503311958,
    -12.271262584796501,
)
MONIC = tuple(c / SINE[-1] for c in SINE[:-1])
LEADING = -SINE[-1] / (14.0 * math.pi)


def params(**more):
    return pltpu.CompilerParams(vmem_limit_bytes=62 * 1024 * 1024, **more)


def place():
    dp, tensor = lax.axis_index("dp"), lax.axis_index("tensor")
    zl, x = dp // 4, dp % 4
    zh, y, c = tensor // 16, (tensor // 2) % 8, tensor % 2
    return dp, tensor, zl, x, zh, y, c


def others(*sizes):
    offsets = [o for o in itertools.product(*(range(n) for n in sizes)) if any(o)]
    return sorted(offsets, key=lambda o: -sum(min(i, n - i) for i, n in zip(o, sizes)))


def plane_peer(dz, dx):
    dp, tensor, zl, x, zh, y, c = place()
    z = (zh * 4 + zl + dz) % 8
    return {"dp": (z % 4) * 4 + (x + dx) % 4, "tensor": ((z // 4) * 8 + y) * 2 + c}


def dp_peer(dz, dx):
    dp, tensor, zl, x, zh, y, c = place()
    return {"dp": ((zl + dz) % 4) * 4 + (x + dx) % 4, "tensor": tensor}


def line_peer(dy, dc):
    dp, tensor, zl, x, zh, y, c = place()
    return {"dp": dp, "tensor": (zh * 8 + (y + dy) % 8) * 2 + (c + dc) % 2}


def remote(src, dst, send, recv, peer):
    return pltpu.make_async_remote_copy(
        src_ref=src, dst_ref=dst, send_sem=send, recv_sem=recv, device_id=peer, device_id_type=MESH
    )


def pick(expert_ref, ids_ref, block_ref, loads, routed_ref, sums_ref):
    tokens, width = block_ref.shape
    hit = jnp.any(ids_ref[...] == expert_ref[0], axis=0, keepdims=True)
    hit = jnp.broadcast_to(jnp.where(hit, 1.0, 0.0), (8, tokens)).astype(jnp.bfloat16)
    up_to = lax.broadcasted_iota(jnp.int32, (tokens, tokens), 0) <= lax.broadcasted_iota(
        jnp.int32, (tokens, tokens), 1
    )
    place_of = jnp.dot(hit, jnp.where(up_to, 1.0, 0.0).astype(jnp.bfloat16), preferred_element_type=jnp.float32)
    slots = lax.broadcasted_iota(jnp.int32, (CAP, tokens), 0).astype(jnp.float32) + 1.0
    wanted = jnp.where(place_of[:1] == slots, hit[:1].astype(jnp.float32), 0.0)
    one_hot = wanted.astype(jnp.bfloat16)
    part = width // len(loads)
    for k, load in enumerate(loads):
        load.wait()
        at = pl.ds(k * part, part)
        rows = jnp.dot(one_hot, block_ref[:, at], preferred_element_type=jnp.float32)
        routed_ref[:, at] = rows.astype(jnp.bfloat16)
        sums_ref[:, at] = jnp.sum(jnp.abs(rows), axis=0, keepdims=True)
    sums_ref[:, width:] = jnp.broadcast_to(jnp.sum(wanted), (1, 128))


def errors_of(w7, aw, s, rs):
    t = jnp.max(aw * s, axis=1, keepdims=True) + 1e-6
    u = (w7 * s) * (1.0 / t)
    x = u - jnp.round(u)
    z = x * x
    p = z + MONIC[-1]
    for c in MONIC[-2::-1]:
        p = p * z + c
    return ((x * t) * rs * p).astype(jnp.bfloat16)


def kernel(
    expert_ref, ratio_ref, ids_ref, block_hbm, w_hbm, col_ref, losses_ref, best_ref,
    block_ref, w_ref, gath, wg, zsum, xsum, aw, w7, s_ref, rs_ref, err, acc, parts, plane, line,
    load_sem,
    zs_send, zs_recv, xs_send, xs_recv, a_send, a_recv, b_send, b_recv, f_send, f_recv,
    g_send, g_recv, d_send, d_recv, p_send, p_recv, l_send, l_recv, m_send, m_recv,
):
    dp, tensor, zl, x, zh, y, c = place()
    depth = block_ref.shape[1]
    slab, cols = w_ref.shape[0], w_ref.shape[1] // 4
    half = depth // 2
    sibling = line_peer(0, 1)
    part = depth // 4
    loads = [
        pltpu.make_async_copy(block_hbm.at[:, pl.ds(k * part, part)], block_ref.at[:, pl.ds(k * part, part)], load_sem.at[k])
        for k in range(4)
    ]
    weights = pltpu.make_async_copy(w_hbm, w_ref, load_sem.at[4])
    for load in loads + [weights]:
        load.start()
    peers = [plane_peer(*o) for o in others(8, 4)] + [line_peer(*o) for o in others(8, 2)]
    barrier = pltpu.get_barrier_semaphore()
    for peer in peers:
        pl.semaphore_signal(barrier, inc=1, device_id=peer, device_id_type=MESH)

    def rows_of(block):
        return pl.ds(pl.multiple_of(block * CAP, 16), CAP)

    pick(expert_ref, ids_ref, block_ref, loads, gath.at[rows_of(zl)], zsum.at[zl])
    pl.semaphore_wait(barrier, len(peers))

    sums = [remote(zsum.at[zl], zsum.at[zl], zs_send.at[k], zs_recv.at[k], plane_peer(dz, 0)) for k, dz in enumerate((2, 1, 7))]
    for copy in sums:
        copy.start()
    weights.wait()
    along = []
    for k, dz in enumerate((1, 3, 2)):
        columns = pl.ds(pl.multiple_of(((zl + dz) % 4) * cols, cols), cols)
        along.append(remote(w_ref.at[:, columns], wg.at[x, zl], a_send.at[k], a_recv.at[k], dp_peer(dz, 0)))
        along[-1].start()
    wg[x, zl] = w_ref[:, pl.ds(pl.multiple_of(zl * cols, cols), cols)]
    beyond = {}

    def across(j):
        held = wg.at[x, (zl + j) % 4]
        for k, dx in enumerate((1, 3)):
            beyond[j, dx] = remote(held, held, b_send.at[2 * j + k], b_recv.at[2 * j + k], dp_peer(0, dx))
            beyond[j, dx].start()

    for copy in sums:
        copy.wait_recv()
    xsum[x] = ((zsum[0] + zsum[1]) + zsum[2]) + zsum[3]
    over = [remote(xsum.at[x], xsum.at[x], xs_send.at[k], xs_recv.at[k], dp_peer(0, dx)) for k, dx in enumerate((2, 1, 3))]
    for copy in over:
        copy.start()
    across(0)
    acc[...] = jnp.zeros_like(acc)
    for k, dz in ((0, 1), (1, 3), (2, 2)):
        along[k].wait_recv()
        across((4 - dz) % 4)

    rows = []
    low = c * half
    for k, (dz, start, size) in enumerate(((1, 0, half), (7, 0, half), (2, 0, half // 2), (6, half // 2, half // 2))):
        at = pl.ds(pl.multiple_of(low + start, GROUP), size)
        held = gath.at[rows_of(zl), at]
        rows.append(remote(held, held, g_send.at[k], g_recv.at[k], plane_peer(dz, 0)))
        rows[-1].start()

    def turn(column):
        for i in range(4):
            for h in range(slab // GROUP):
                tile = wg[column, i, h * GROUP : (h + 1) * GROUP, :].astype(jnp.float32).T
                at = pl.ds(pl.multiple_of((i * 4 + column) * slab + h * GROUP, GROUP), GROUP)
                aw[:, at] = jnp.abs(tile)
                w7[:, at] = 7.0 * tile

    def fill(column, first, last):
        def step(pair, _):
            for one in range(2):
                r = pair * 2 + one
                for i in range(4):
                    for h in range(slab // GROUP):
                        group = (i * 4 + column) * (slab // GROUP) + h
                        at = pl.ds(pl.multiple_of(group * GROUP, GROUP), GROUP)
                        err[group, pl.ds(pl.multiple_of(r * cols, cols), cols), :] = errors_of(
                            w7[:, at], aw[:, at], s_ref[r, :, at], rs_ref[r, :, at]
                        )
            return 0

        lax.fori_loop(first, last, step, 0)

    turn(x)
    for copy in over:
        copy.wait_recv()
    total = ((xsum[0] + xsum[1]) + xsum[2]) + xsum[3]
    logs = jnp.log(0.001 + total[:, :depth])
    count = total[:, depth:]
    for r in range(RATIOS):
        s = jnp.exp((ratio_ref[r].astype(jnp.float32) / GRID) * logs)
        s_ref[r] = s
        rs_ref[r] = LEADING / s

    fill(x, 0, 3)
    onward = []
    behind, ahead = (x + 3) % 4, (x + 1) % 4
    for k, (j, dx, column) in enumerate(((0, 1, behind), (1, 1, behind), (2, 3, ahead), (3, 3, ahead))):
        beyond[j, dx].wait_recv()
        held = wg.at[column, (zl + j) % 4]
        onward.append(remote(held, held, f_send.at[k], f_recv.at[k], dp_peer(0, dx)))
        onward[-1].start()
    fill(x, 3, RATIOS // 2)
    for j in (2, 3):
        beyond[j, 1].wait_recv()
    turn(behind)
    fill(behind, 0, RATIOS // 2)
    for j in (0, 1):
        beyond[j, 3].wait_recv()
    turn(ahead)
    fill(ahead, 0, RATIOS // 2)
    mine = pl.ds(pl.multiple_of(low, GROUP), half)
    passed = []

    def pass_on(k, arrived, back):
        for one in arrived:
            rows[one].wait_recv()
        held = gath.at[rows_of((zl + back) % 4), mine]
        passed.append(remote(held, held, d_send.at[k], d_recv.at[k], sibling))
        passed[-1].start()

    pass_on(0, (0,), 3)
    pass_on(1, (1,), 1)
    for copy in onward:
        copy.wait_recv()
    far = (x + 2) % 4
    turn(far)
    fill(far, 0, 3)
    pass_on(2, (2, 3), 2)
    fill(far, 3, RATIOS // 2)
    def multiply(k, _):
        chunk = (k + 2 * c) % 4
        at = pl.ds(pl.multiple_of(chunk * part, part), part)
        groups = part // GROUP
        errors = jnp.concatenate([err[chunk * groups + j] for j in range(groups)], axis=1)
        acc[...] += lax.dot_general(
            gath[:, at], errors, (((1,), (1,)), ((), ())), preferred_element_type=jnp.float32
        )
        return 0

    lax.fori_loop(0, 2, multiply, 0)
    for copy in passed:
        copy.wait_recv()
    lax.fori_loop(2, 4, multiply, 0)
    factor = LOSS_SCALE / count
    own = parts.at[dp]
    for r in range(RATIOS):
        a = acc[:, r * cols : (r + 1) * cols]
        own[r : r + 1, :] = factor * jnp.sum(a * a, axis=0, keepdims=True)
    own[RATIOS:, :] = jnp.zeros((16 - RATIOS, cols), jnp.float32)

    pieces = [remote(own, own, p_send.at[k], p_recv.at[k], dp_peer(*o)) for k, o in enumerate(others(4, 4))]
    diagonal = lax.broadcasted_iota(jnp.int32, (16, 128), 0) == lax.broadcasted_iota(jnp.int32, (16, 128), 1)
    row = plane.at[(zh * 4 + zl) * 4 + x]
    row[...] = jnp.sum(jnp.where(diagonal, jnp.sum(own[...], axis=1, keepdims=True), 0.0), axis=0, keepdims=True)
    shares = [remote(row, row, l_send.at[k], l_recv.at[k], plane_peer(*o)) for k, o in enumerate(others(8, 4))]
    for copy in shares + pieces:
        copy.start()
    for copy in shares:
        copy.wait_recv()
    row = line.at[y * 2 + c]
    row[...] = jnp.sum(plane[...], axis=0)
    ends = [remote(row, row, m_send.at[k], m_recv.at[k], line_peer(*o)) for k, o in enumerate(others(8, 2))]
    for copy in ends:
        copy.start()
    for copy in pieces:
        copy.wait_recv()
    for q in range(4):
        piece = ((parts[4 * q] + parts[4 * q + 1]) + parts[4 * q + 2]) + parts[4 * q + 3]
        col_ref[:, q * cols : (q + 1) * cols] = piece[:RATIOS]
    for copy in ends:
        copy.wait_recv()
    losses = jnp.sum(line[...], axis=0) / FF
    losses_ref[...] = losses
    lane = lax.broadcasted_iota(jnp.int32, (1, 128), 1)
    best = jnp.min(jnp.where(lane < RATIOS, losses, jnp.inf), axis=1, keepdims=True)
    best_ref[...] = jnp.broadcast_to(best, (1, 128))
    for copy in sums + along + list(beyond.values()) + rows + over + onward + passed + pieces + shares + ends:
        copy.wait_send()


def finish_kernel(col_ref, losses_ref, best_ref, col_out, losses_out, best_out):
    col_out[...] = col_ref[...]
    for r in range(RATIOS):
        losses_out[r] = losses_ref[0, r]
    best_out[0] = best_ref[0, 0]


def body(calibration, expert_ids, chosen_expert, ratio_ids, gate_weight):
    f32, bf16 = jnp.float32, jnp.bfloat16
    width = calibration.shape[1]
    slab, cols = gate_weight.shape
    long, cols = width + 128, cols // 4
    col_loss, losses, best = pl.pallas_call(
        kernel,
        out_shape=[
            jax.ShapeDtypeStruct((RATIOS, 4 * cols), f32),
            jax.ShapeDtypeStruct((1, 128), f32),
            jax.ShapeDtypeStruct((1, 128), f32),
        ],
        in_specs=[SMEM, SMEM, VMEM, ANY, ANY],
        out_specs=[VMEM] * 3,
        scratch_shapes=[
            pltpu.VMEM(calibration.shape, bf16),
            pltpu.VMEM((slab, 4 * cols), bf16),
            pltpu.VMEM((4 * CAP, width), bf16),
            pltpu.VMEM((4, 4, slab, cols), bf16),
            pltpu.VMEM((4, 1, long), f32),
            pltpu.VMEM((4, 1, long), f32),
            pltpu.VMEM((cols, width), f32),
            pltpu.VMEM((cols, width), f32),
            pltpu.VMEM((RATIOS, 1, width), f32),
            pltpu.VMEM((RATIOS, 1, width), f32),
            pltpu.VMEM((width // GROUP, RATIOS * cols, GROUP), bf16),
            pltpu.VMEM((4 * CAP, RATIOS * cols), f32),
            pltpu.VMEM((16, 16, cols), f32),
            pltpu.VMEM((32, 1, 128), f32),
            pltpu.VMEM((16, 1, 128), f32),
        ]
        + [DMA((n,)) for n in (5, 3, 3, 3, 3, 3, 3, 8, 8, 4, 4, 4, 4, 3, 3, 15, 15, 31, 31, 15, 15)],
        compiler_params=params(collective_id=0, has_side_effects=True),
        name="search",
    )(chosen_expert, ratio_ids, expert_ids.T, calibration, gate_weight)
    return pl.pallas_call(
        finish_kernel,
        out_shape=[
            jax.ShapeDtypeStruct((RATIOS, 4 * cols), f32),
            jax.ShapeDtypeStruct((RATIOS,), f32),
            jax.ShapeDtypeStruct((1,), f32),
        ],
        in_specs=[VMEM, SMEM, SMEM],
        out_specs=[VMEM, SMEM, SMEM],
        name="finish",
    )(col_loss, losses, best)


def solution(mesh):
    placed = (P("dp", None), P("dp", None), P(), P(), P("dp", "tensor"))
    return jax.shard_map(
        body, mesh=mesh, in_specs=placed, out_specs=(P(None, "tensor"), P(), P()), check_vma=False
    )
```
